256 devices in a mesh: gx: 4 (over x), gy: 4 (over y_lo, core), zt: 16 (over y_hi, z).
Axes of the slice: x: 4, y: 4 (y_hi: 2, y_lo: 2; y = y_hi * 2 + y_lo), z: 8, core: 2. Of those that a mesh axis runs over, the one named last changes fastest.
Arguments:
- gauge_links: float32 [4, 2, 3, 3, 8, 32, 2048], P(None, None, None, None, 'gx', 'gy', 'zt'), may hold values from -1 to 1, as said below
- momenta: float32 [4, 2, 3, 3, 8, 32, 2048], P(None, None, None, None, 'gx', 'gy', 'zt'), may hold values from -4 to 4, as said below
Outputs:
- new_links: float32 [4, 2, 3, 3, 8, 32, 2048], P(None, None, None, None, 'gx', 'gy', 'zt')
- new_momenta: float32 [4, 2, 3, 3, 8, 32, 2048], P(None, None, None, None, 'gx', 'gy', 'zt')
- plaquette: float32 [], replicated
The draws below stay inside these ranges and needn't reach their ends.
Inputs may be any that keep to these rules, and one draw needn't show every extreme that they name: `gauge_links`: every link is a unitary 3 x 3 complex matrix. `momenta`: every momentum is an antihermitian traceless 3 x 3 complex matrix.
All inputs are finite; a program needn't handle non-finite values.
Results may differ from the reference program's by a relative error of at most 0.0001.
Values sent between devices are 32-bit elements; how exact they have to be, the bound alone decides.
A program may use at most 128 MiB of HBM per device.

```python
import jax
import jax.numpy as jnp

LT = 64
NX = 8
NY = 32
NZ = 32


def times_pair(first, second):
    return (first[0] * second[0] - first[1] * second[1], first[0] * second[1] + first[1] * second[0])


def unitary_from(real_gen, imag_gen):
    identity = jnp.eye(3, dtype=jnp.float32)[:, :, None, None, None, None]
    top_real = identity + 0.5 * real_gen
    top_imag = 0.5 * imag_gen
    low_real = identity - 0.5 * real_gen
    low_imag = -0.5 * imag_gen

    def element(row_index, column):
        return (low_real[row_index % 3, column % 3], low_imag[row_index % 3, column % 3])
    cofactor = []
    for row_index in range(3):
        line = []
        for column in range(3):
            first = times_pair(element(column + 1, row_index + 1), element(column + 2, row_index + 2))
            second = times_pair(element(column + 1, row_index + 2), element(column + 2, row_index + 1))
            line.append((first[0] - second[0], first[1] - second[1]))
        cofactor.append(line)
    determinant = times_pair(element(0, 0), cofactor[0][0])
    for middle in (1, 2):
        extra = times_pair(element(0, middle), cofactor[middle][0])
        determinant = (determinant[0] + extra[0], determinant[1] + extra[1])
    norm_square = determinant[0] * determinant[0] + determinant[1] * determinant[1]
    inverse_det = (determinant[0] / norm_square, -determinant[1] / norm_square)
    real_rows = []
    imag_rows = []
    for row_index in range(3):
        real_line = []
        imag_line = []
        for column in range(3):
            total_real = 0.0
            total_imag = 0.0
            for inner in range(3):
                entry = times_pair(cofactor[inner][column], inverse_det)
                value = times_pair((top_real[row_index, inner], top_imag[row_index, inner]), entry)
                total_real = total_real + value[0]
                total_imag = total_imag + value[1]
            real_line.append(total_real)
            imag_line.append(total_imag)
        real_rows.append(jnp.stack(real_line))
        imag_rows.append(jnp.stack(imag_line))
    return (jnp.stack(real_rows), jnp.stack(imag_rows))


def draw_gauge_links(key, part):
    key_x = jax.random.fold_in(key, 11)
    key_z = jax.random.fold_in(key, 12)
    key_noise = jax.random.fold_in(key, 13)
    order_x = jax.random.uniform(key_x, (NX,), jnp.float32)
    order_z = jax.random.uniform(key_z, (NZ,), jnp.float32)
    strength = 0.4 + 3.0 * order_x[:, None, None, None] * order_z[None, None, :, None]
    strength = jnp.broadcast_to(strength, (NX, NY, NZ, LT)).reshape(NX, NY, NZ * LT)
    shape = (2, 3, 3, 4, NX, NY, NZ * LT)
    noise = jax.random.normal(key_noise, shape, jnp.float32)
    identity = jnp.eye(3, dtype=jnp.float32)[:, :, None, None, None, None]
    real_gen = 0.5 * (noise[0] - jnp.swapaxes(noise[0], 0, 1)) * strength
    imag_sym = 0.5 * (noise[1] + jnp.swapaxes(noise[1], 0, 1))
    trace_imag = (imag_sym[0, 0] + imag_sym[1, 1] + imag_sym[2, 2]) / 3.0
    imag_gen = (imag_sym - trace_imag * identity) * strength
    real_link, imag_link = unitary_from(real_gen, imag_gen)
    result = jnp.stack([real_link, imag_link])
    result = jnp.moveaxis(result, 3, 0)
    return jnp.clip(result, -1.0, 1.0).astype(jnp.float32)


def draw_momenta(key, part):
    key_base = jax.random.fold_in(key, 21)
    shape = (4, 2, 3, 3, NX, NY, NZ * LT)
    base = jax.random.truncated_normal(key_base, -3.0, 3.0, shape, jnp.float32)
    identity = jnp.eye(3, dtype=jnp.float32)[:, :, None, None, None]
    real_part = 0.5 * (base[:, 0] - jnp.swapaxes(base[:, 0], 1, 2))
    imag_part = 0.5 * (base[:, 1] + jnp.swapaxes(base[:, 1], 1, 2))
    trace_imag = (imag_part[:, 0, 0] + imag_part[:, 1, 1] + imag_part[:, 2, 2]) / 3.0
    imag_part = imag_part - trace_imag[:, None, None] * identity
    return jnp.stack([real_part, imag_part], axis=1).astype(jnp.float32)


def setup_inputs(seed: int = 0) -> dict:
    keys = jax.random.split(jax.random.key(seed), 3)
    gauge_links = draw_gauge_links(jax.random.fold_in(keys[2], 71), 0)
    momenta = draw_momenta(jax.random.fold_in(keys[2], 71), 0)
    return dict(gauge_links=gauge_links, momenta=momenta)


kick_size = 0.25
step_size = 0.2


def matrix_product(left, right):
    real_part = 0.0
    imag_part = 0.0
    for inner in range(3):
        left_real = left[0][:, inner:inner + 1]
        left_imag = left[1][:, inner:inner + 1]
        right_real = right[0][inner:inner + 1]
        right_imag = right[1][inner:inner + 1]
        real_part = real_part + (left_real * right_real - left_imag * right_imag)
        imag_part = imag_part + (left_real * right_imag + left_imag * right_real)
    return jnp.stack([real_part, imag_part])


def adjoint(matrix):
    return jnp.stack([jnp.swapaxes(matrix[0], 0, 1), -jnp.swapaxes(matrix[1], 0, 1)])


def traceless_part(matrix):
    identity = jnp.eye(3, dtype=jnp.float32)[:, :, None, None, None]
    real_part = 0.5 * (matrix[0] - jnp.swapaxes(matrix[0], 0, 1))
    imag_part = 0.5 * (matrix[1] + jnp.swapaxes(matrix[1], 0, 1))
    trace_imag = (matrix[1][0, 0] + matrix[1][1, 1] + matrix[1][2, 2]) / 3.0
    return jnp.stack([real_part, imag_part - trace_imag * identity])


def complex_times(first, second):
    return (first[0] * second[0] - first[1] * second[1], first[0] * second[1] + first[1] * second[0])


def cayley(matrix):
    identity = jnp.eye(3, dtype=jnp.float32)[:, :, None, None, None]
    numerator = jnp.stack([identity + 0.5 * matrix[0], 0.5 * matrix[1]])
    denominator = jnp.stack([identity - 0.5 * matrix[0], -0.5 * matrix[1]])

    def element(row_index, column):
        return (denominator[0, row_index % 3, column % 3], denominator[1, row_index % 3, column % 3])

    cofactor = []
    for row_index in range(3):
        line = []
        for column in range(3):
            first = complex_times(element(column + 1, row_index + 1), element(column + 2, row_index + 2))
            second = complex_times(element(column + 1, row_index + 2), element(column + 2, row_index + 1))
            line.append((first[0] - second[0], first[1] - second[1]))
        cofactor.append(line)
    determinant = complex_times(element(0, 0), cofactor[0][0])
    for middle in (1, 2):
        extra = complex_times(element(0, middle), cofactor[middle][0])
        determinant = (determinant[0] + extra[0], determinant[1] + extra[1])
    norm_square = determinant[0] * determinant[0] + determinant[1] * determinant[1]
    inverse_det = (determinant[0] / norm_square, -determinant[1] / norm_square)
    real_rows = []
    imag_rows = []
    for row_index in range(3):
        values = [complex_times(cofactor[row_index][column], inverse_det) for column in range(3)]
        real_rows.append(jnp.stack([value[0] for value in values]))
        imag_rows.append(jnp.stack([value[1] for value in values]))
    inverse = jnp.stack([jnp.stack(real_rows), jnp.stack(imag_rows)])
    return matrix_product(numerator, inverse)


def roll_time(matrix, steps):
    shape = matrix.shape
    folded = matrix.reshape(shape[:-1] + (shape[-1] // LT, LT))
    return jnp.roll(folded, -steps, axis=-1).reshape(shape)


def displaced(matrix, direction, steps):
    if direction == 0:
        return jnp.roll(matrix, -steps, axis=-3)
    if direction == 1:
        return jnp.roll(matrix, -steps, axis=-2)
    if direction == 2:
        return jnp.roll(matrix, -steps * LT, axis=-1)
    return roll_time(matrix, steps)


def staple_sums(link_list):
    result = []
    for along in range(4):
        staple = None
        for across in range(4):
            if across == along:
                continue
            ahead_across = displaced(link_list[across], along, 1)
            upper_staple = matrix_product(matrix_product(ahead_across, adjoint(displaced(link_list[along], across, 1))), adjoint(link_list[across]))
            lower_staple = matrix_product(matrix_product(adjoint(ahead_across), adjoint(link_list[along])), link_list[across])
            term = upper_staple + displaced(lower_staple, across, -1)
            staple = term if staple is None else staple + term
        result.append(staple)
    return result


def reference(gauge_links, momenta):
    link_list = [gauge_links[index] for index in range(4)]
    first_staples = staple_sums(link_list)
    half_momenta = []
    new_list = []
    for along in range(4):
        gauge_force = traceless_part(matrix_product(link_list[along], first_staples[along]))
        half_step = momenta[along] - kick_size * gauge_force
        half_momenta.append(half_step)
        new_list.append(matrix_product(cayley(step_size * traceless_part(half_step)), link_list[along]))
    second_staples = staple_sums(new_list)
    final_momenta = []
    trace_total = jnp.float32(0.0)
    for along in range(4):
        loop_matrix = matrix_product(new_list[along], second_staples[along])
        final_momenta.append(half_momenta[along] - kick_size * traceless_part(loop_matrix))
        trace_total = trace_total + jnp.sum(loop_matrix[0][0, 0] + loop_matrix[0][1, 1] + loop_matrix[0][2, 2])
    plaquette = trace_total / (72.0 * NX * NY * NZ * LT)
    return (jnp.stack(new_list), jnp.stack(final_momenta), plaquette)
```

```python
import jax
import jax.numpy as jnp
from jax import lax
from jax.experimental import pallas as pl
from jax.experimental.pallas import tpu as pltpu
from jax.sharding import PartitionSpec as P

MESH = pl.DeviceIdType.MESH
F32 = jnp.float32
KICK = 0.25
STEP = 0.2
NAMES = ("gx", "gy", "zt")
LEAD = {(0, 1): 1, (0, 2): 2, (0, 3): 3, (1, 2): 2, (1, 3): 1, (2, 3): 2}
OTHER = (lambda k: k + 1, lambda k: k + (k + 1) // 2, lambda k: k + k // 2, lambda k: k)


def load_matrix(ref, lead, x):
    return [[(ref[lead + (3 * i + j, x)], ref[lead + (9 + 3 * i + j, x)]) for j in range(3)] for i in range(3)]


def add(a, b):
    return b if a is None else a + b


def product(a, b):
    out = []
    for i in range(3):
        line = []
        for j in range(3):
            re, im = None, None
            for k in range(3):
                ar, ai = a[i][k]
                br, bi = b[k][j]
                re = add(re, ar * br - ai * bi)
                im = add(im, ar * bi + ai * br)
            line.append((re, im))
        out.append(line)
    return out


def dagger_entry(x, y, i, j):
    re, im = None, None
    for k in range(3):
        ar, ai = x[i][k]
        br, bi = y[j][k]
        re = add(re, ar * br + ai * bi)
        im = add(im, ai * br - ar * bi)
    return re, im


def twice_traceless(x, y):
    diag = []
    for i in range(3):
        im = None
        for k in range(3):
            ar, ai = x[i][k]
            br, bi = y[i][k]
            im = add(im, ai * br - ar * bi)
        diag.append(im)
    mean = (diag[0] + diag[1] + diag[2]) * (2.0 / 3.0)
    out = [diag[0] + diag[0] - mean, diag[1] + diag[1] - mean]
    for i, j in ((0, 1), (0, 2), (1, 2)):
        pr, pi = dagger_entry(x, y, i, j)
        qr, qi = dagger_entry(x, y, j, i)
        out += [pr - qr, pi + qi]
    return out


def real_trace(x, y):
    total = None
    for i in range(3):
        for k in range(3):
            ar, ai = x[i][k]
            br, bi = y[i][k]
            total = add(total, ar * br + ai * bi)
    return total


def conjugated(d, t):
    d0, d1, ur, ui, vr, vi, wr, wi = t
    d2 = -(d0 + d1)

    def column(j):
        (ar, ai), (br, bi), (cr, ci) = d[0][j], d[1][j], d[2][j]
        first = (
            ur * br - ui * bi + (vr * cr - vi * ci) - d0 * ai,
            ur * bi + ui * br + (vr * ci + vi * cr) + d0 * ar,
        )
        second = (
            wr * cr - wi * ci - (ur * ar + ui * ai) - d1 * bi,
            wr * ci + wi * cr + (ui * ar - ur * ai) + d1 * br,
        )
        third = (
            -(vr * ar + vi * ai) - (wr * br + wi * bi) - d2 * ci,
            (vi * ar - vr * ai) + (wi * br - wr * bi) + d2 * cr,
        )
        return first, second, third

    def imag(i, col):
        total = None
        for k in range(3):
            ar, ai = d[k][i]
            total = add(total, ar * col[k][1] - ai * col[k][0])
        return total

    def entry(i, col):
        re, im = None, None
        for k in range(3):
            ar, ai = d[k][i]
            br, bi = col[k]
            re = add(re, ar * br + ai * bi)
            im = add(im, ar * bi - ai * br)
        return re, im

    zero = column(0)
    e0 = imag(0, zero)
    one = column(1)
    e1 = imag(1, one)
    u = entry(0, one)
    two = column(2)
    v = entry(0, two)
    w = entry(1, two)
    return [e0, e1, u[0], u[1], v[0], v[1], w[0], w[1]]


def cayley(h, scale):
    a0, a1, ur, ui, vr, vi, wr, wi = [scale * part for part in h]
    a2 = -(a0 + a1)
    uu = ur * ur + ui * ui
    vv = vr * vr + vi * vi
    ww = wr * wr + wi * wi
    s00, s11, s22 = a0 * a0, a1 * a1, a2 * a2
    one_s = 1.0 + (0.5 * (s00 + s11 + s22) + (uu + vv + ww))
    uwr, uwi = ur * wr - ui * wi, ur * wi + ui * wr
    det_h = a0 * a1 * a2 + 2.0 * (uwi * vr - uwr * vi) - a0 * ww - a1 * vv - a2 * uu
    scale2 = 2.0 / (one_s * one_s + det_h * det_h)
    qr, qi = one_s * scale2, -(det_h * scale2)
    pr, pi = a2 * ui - (vr * wr + vi * wi), -(a2 * ur) - (vi * wr - vr * wi)
    rr, ri = a1 * vi + uwr, uwi - a1 * vr
    tr, ti = a0 * wi - (ur * vr + ui * vi), -(a0 * wr) - (ur * vi - ui * vr)
    rows = [
        [(one_s - (s00 + uu + vv), a0), (ur + pr, ui + pi), (vr + rr, vi + ri)],
        [(pr - ur, ui - pi), (one_s - (s11 + uu + ww), a1), (wr + tr, wi + ti)],
        [(rr - vr, vi - ri), (tr - wr, wi - ti), (one_s - (s22 + vv + ww), a2)],
    ]
    out = []
    for i in range(3):
        line = []
        for j in range(3):
            br, bi = rows[i][j]
            re, im = br * qr - bi * qi, br * qi + bi * qr
            line.append((re - 1.0 if i == j else re, im))
        out.append(line)
    return out


PARTS = (9, 13, 1, 10, 2, 11, 5, 14)


def kernel(
    sizes, gauge, momenta, new_links, new_momenta, plaquette,
    links, shifted, row_out, row_in, lane_out, lane_in,
    loops, lower, low_row_out, low_row_in, low_lane_out, low_lane_in,
    moment, final, traces, gather,
    load_sem, x_send, x_recv, y_send, y_recv, z_send, z_recv,
    lx_send, lx_recv, ly_send, ly_recv, lz_send, lz_recv, sum_send, sum_recv, store_sem,
):
    me = [lax.axis_index(name) for name in NAMES]

    def peer(axis, offset):
        return {NAMES[axis]: lax.rem(me[axis] + (offset + sizes[axis]), sizes[axis])}

    barrier = pltpu.get_barrier_semaphore()
    count = 0
    for axis in range(3):
        for offset in range(1, sizes[axis]):
            pl.semaphore_signal(barrier, inc=1, device_id=peer(axis, offset), device_id_type=MESH)
            count += 1

    loads = []
    for m in range(4):
        loads.append(pltpu.make_async_copy(gauge.at[m], links.at[0, m], load_sem.at[m]))
    for n in (1, 2, 3):
        loads.append(pltpu.make_async_copy(gauge.at[n, :, 1], shifted.at[0, 0, n, :, 0], load_sem.at[3 + n]))
    loads.append(pltpu.make_async_copy(momenta, moment, load_sem.at[7]))
    for copy in loads:
        copy.start()

    lane = lax.broadcasted_iota(jnp.int32, (8, 128), 1)
    row = lax.broadcasted_iota(jnp.int32, (8, 128), 0)
    low = lane < 64
    time = lax.rem(lane, 64)
    last_time = time == 63
    first_time = time == 0
    last_row = row == 7
    first_row = row == 0

    for copy in loads[:4]:
        copy.wait()

    def x_copy(ph, n):
        return pltpu.make_async_remote_copy(
            src_ref=links.at[ph, n, :, 0], dst_ref=shifted.at[ph, 0, n, :, 1],
            send_sem=x_send.at[ph, n], recv_sem=x_recv.at[ph, n],
            device_id=peer(0, -1), device_id_type=MESH)

    def y_copy(ph):
        return pltpu.make_async_remote_copy(
            src_ref=row_out.at[ph], dst_ref=row_in.at[ph],
            send_sem=y_send.at[ph], recv_sem=y_recv.at[ph],
            device_id=peer(1, -1), device_id_type=MESH)

    def z_copy(ph, k):
        return pltpu.make_async_remote_copy(
            src_ref=lane_out.at[ph, k], dst_ref=lane_in.at[ph, k],
            send_sem=z_send.at[ph, k], recv_sem=z_recv.at[ph, k],
            device_id=peer(2, -1), device_id_type=MESH)

    def lx_copy(ph, m):
        return pltpu.make_async_remote_copy(
            src_ref=lower.at[ph, 0, m, :, 2], dst_ref=lower.at[ph, 0, m, :, 0],
            send_sem=lx_send.at[ph, m], recv_sem=lx_recv.at[ph, m],
            device_id=peer(0, 1), device_id_type=MESH)

    def ly_copy(ph):
        return pltpu.make_async_remote_copy(
            src_ref=low_row_out.at[ph], dst_ref=low_row_in.at[ph],
            send_sem=ly_send.at[ph], recv_sem=ly_recv.at[ph],
            device_id=peer(1, 1), device_id_type=MESH)

    def lz_copy(ph, k):
        return pltpu.make_async_remote_copy(
            src_ref=low_lane_out.at[ph, k], dst_ref=low_lane_in.at[ph, k],
            send_sem=lz_send.at[ph, k], recv_sem=lz_recv.at[ph, k],
            device_id=peer(2, 1), device_id_type=MESH)

    def plane(ph, m, n, x, slot):
        a = load_matrix(links, (ph, m), x)
        b = load_matrix(shifted, (ph, m, n), x)
        left = product(a, b)
        d = load_matrix(links, (ph, n), x)
        c = load_matrix(shifted, (ph, n, m), x)
        right = product(d, c)
        t = twice_traceless(left, right)
        if ph == 1:
            traces[slot] = real_trace(left, right)
        for p in range(8):
            loops[m, n, p, x] = t[p]
        for p, value in enumerate(conjugated(d, t)):
            lower[ph, n, m, p, x + 1] = value
        for p, value in enumerate(conjugated(a, t)):
            lower[ph, m, n, p, x + 1] = value

    def pairs(body):
        def step(i, _):
            body(i // 2, lax.rem(i, 2))
            return 0
        lax.fori_loop(0, 6, step, 0)

    def sum_copy(axis, offset):
        return pltpu.make_async_remote_copy(
            src_ref=gather.at[axis, me[axis]], dst_ref=gather.at[axis, me[axis]],
            send_sem=sum_send.at[axis, offset], recv_sem=sum_recv.at[axis, offset],
            device_id=peer(axis, offset), device_id_type=MESH)

    for ph in range(2):
        def pack_rows(k, x):
            n = OTHER[1](k)
            for c in range(18):
                row_out[ph, k, c, x] = links[ph, n, c, x, 0:1, :]
        pairs(pack_rows)

        def pack_lanes(k, _):
            n = OTHER[2](k)
            for c in range(18):
                v0 = links[ph, n, c, 0]
                v1 = links[ph, n, c, 1]
                r0 = pltpu.roll(v0, 64, 1)
                lane_out[ph, k, c] = jnp.where(low, v1, r0)
                shifted[ph, 2, n, c, 0] = r0
                shifted[ph, 2, n, c, 1] = pltpu.roll(v1, 64, 1)
            return 0
        lax.fori_loop(0, 3, pack_lanes, 0)

        if ph == 0:
            pl.semaphore_wait(barrier, count)
        for n in (1, 3, 2):
            x_copy(ph, n).start()
        y_copy(ph).start()
        for k in range(3):
            z_copy(ph, k).start()

        def shift_time(k, x):
            for c in range(18):
                v = links[ph, k, c, x]
                shifted[ph, 3, k, c, x] = jnp.where(last_time, pltpu.roll(v, 63, 1), pltpu.roll(v, 127, 1))
        pairs(shift_time)
        if ph == 0:
            for copy in loads[4:7]:
                copy.wait()
        plane(ph, 3, 0, 0, 0)

        y_copy(ph).wait_recv()

        def shift_rows(k, x):
            n = OTHER[1](k)
            for c in range(18):
                v = links[ph, n, c, x]
                edge = jnp.broadcast_to(row_in[ph, k, c, x], (8, 128))
                shifted[ph, 1, n, c, x] = jnp.where(last_row, edge, pltpu.roll(v, 7, 0))
        pairs(shift_rows)

        def y_planes(i, _):
            plane(ph, 1, 3 - 3 * (i // 2), lax.rem(i, 2), 1 + i)
            return 0
        lax.fori_loop(0, 3, y_planes, 0)

        x_copy(ph, 1).wait_recv()
        x_copy(ph, 3).wait_recv()

        def x_planes(i, _):
            plane(ph, 1 + 2 * i, 0, 1, 4 + i)
            return 0
        lax.fori_loop(0, 2, x_planes, 0)
        x_copy(ph, 2).wait_recv()
        for k in range(3):
            z_copy(ph, k).wait_recv()

        def shift_lanes(k, _):
            n = OTHER[2](k)
            for c in range(18):
                edge = lane_in[ph, k, c]
                shifted[ph, 2, n, c, 0] = jnp.where(low, shifted[ph, 2, n, c, 0], edge)
                shifted[ph, 2, n, c, 1] = jnp.where(low, shifted[ph, 2, n, c, 1], pltpu.roll(edge, 64, 1))
            return 0
        lax.fori_loop(0, 3, shift_lanes, 0)

        pairs(lambda k, x: plane(ph, 2, OTHER[2](k), x, 6 + 2 * k + x))

        if ph == 1:
            total = traces[0]
            for slot in range(1, 12):
                total = total + traces[slot]
            gather[0, me[0]] = jnp.sum(total, axis=0, keepdims=True)
            for offset in range(1, sizes[0]):
                sum_copy(0, offset).start()

        for m in (1, 2, 3):
            lx_copy(ph, m).start()

        def pack_low_rows(k, x):
            m = OTHER[1](k)
            for p in range(8):
                low_row_out[ph, k, p, x] = lower[ph, 1, m, p, x + 1, 7:8, :]
        pairs(pack_low_rows)

        def pack_low_lanes(k, _):
            m = OTHER[2](k)
            for p in range(8):
                low_lane_out[ph, k, p] = jnp.where(low, pltpu.roll(lower[ph, 2, m, p, 1], 64, 1), lower[ph, 2, m, p, 2])
            return 0
        lax.fori_loop(0, 3, pack_low_lanes, 0)
        ly_copy(ph).start()
        for k in range(3):
            lz_copy(ph, k).start()

        if ph == 0:
            loads[7].wait()
        ly_copy(ph).wait_recv()
        for m in (1, 2, 3):
            lx_copy(ph, m).wait_recv()
        for k in range(3):
            lz_copy(ph, k).wait_recv()

        def force(x, _):
            for m in range(4):
                total = [None] * 8
                for n in range(4):
                    if n == m:
                        continue
                    lead = LEAD[min(m, n), max(m, n)]
                    first, second = (m, n) if lead == m else (n, m)
                    for p in range(8):
                        here = loops[first, second, p, x]
                        if n == 0:
                            below = lower[ph, 0, m, p, x]
                        else:
                            value = lower[ph, n, m, p, x + 1]
                            if n == 1:
                                k = {0: 0, 2: 1, 3: 2}[m]
                                edge = jnp.broadcast_to(low_row_in[ph, k, p, x], (8, 128))
                                below = jnp.where(first_row, edge, pltpu.roll(value, 1, 0))
                            elif n == 2:
                                k = {0: 0, 1: 1, 3: 2}[m]
                                edge = pltpu.roll(low_lane_in[ph, k, p], 64 * x, 1)
                                below = jnp.where(low, edge, pltpu.roll(value, 64, 1))
                            else:
                                below = jnp.where(first_time, pltpu.roll(value, 65, 1), pltpu.roll(value, 1, 1))
                        term = here - below if lead == m else below - here
                        total[p] = add(total[p], term)
                if ph == 0:
                    for p in range(8):
                        moment[m, PARTS[p], x] = moment[m, PARTS[p], x] - (0.5 * KICK) * total[p]
                else:
                    h = [moment[m, PARTS[p], x] - (0.5 * KICK) * total[p] for p in range(8)]
                    for p in range(8):
                        final[m, PARTS[p], x] = h[p]
                    final[m, 17, x] = -(h[0] + h[1])
                    for c, p in ((3, 2), (6, 4), (7, 6)):
                        final[m, c, x] = -h[p]
                        final[m, 9 + c, x] = h[p + 1]
                    for c in (0, 4, 8):
                        final[m, c, x] = jnp.zeros((8, 128), F32)
            return 0
        lax.fori_loop(0, 2, force, 0)

        if ph == 0:
            def update(i, _):
                m, x = i // 2, lax.rem(i, 2)
                u = cayley([moment[m, p, x] for p in PARTS], 0.5 * STEP)
                new = product(u, load_matrix(links, (0, m), x))
                for i3 in range(3):
                    for j3 in range(3):
                        for part in range(2):
                            links[1, m, 9 * part + 3 * i3 + j3, x] = new[i3][j3][part]
                return 0
            lax.fori_loop(0, 8, update, 0)

            def copy_x(k, _):
                for c in range(18):
                    shifted[1, 0, k + 1, c, 0] = links[1, k + 1, c, 1]
                return 0
            lax.fori_loop(0, 3, copy_x, 0)
            store_links = pltpu.make_async_copy(links.at[1], new_links, store_sem.at[0])
            store_links.start()

    store_momenta = pltpu.make_async_copy(final, new_momenta, store_sem.at[1])
    store_momenta.start()
    for axis in range(3):
        for offset in range(1, sizes[axis]):
            sum_copy(axis, offset).wait_recv()
        total = gather[axis, 0]
        for source in range(1, sizes[axis]):
            total = total + gather[axis, source]
        if axis < 2:
            gather[axis + 1, me[axis + 1]] = total
            for offset in range(1, sizes[axis + 1]):
                sum_copy(axis + 1, offset).start()
    volume = 72.0 * (2 * 8 * 128) * (sizes[0] * sizes[1] * sizes[2])
    plaquette[0, 0] = jnp.sum(total) * (4.0 / volume)

    for ph in range(2):
        for n in (1, 2, 3):
            x_copy(ph, n).wait_send()
            lx_copy(ph, n).wait_send()
        y_copy(ph).wait_send()
        ly_copy(ph).wait_send()
        for k in range(3):
            z_copy(ph, k).wait_send()
            lz_copy(ph, k).wait_send()
    for axis in range(3):
        for offset in range(1, sizes[axis]):
            sum_copy(axis, offset).wait_send()
    store_links.wait()
    store_momenta.wait()


def solution(mesh):
    sizes = tuple(mesh.shape[name] for name in NAMES)
    spec = P(None, None, None, None, "gx", "gy", "zt")

    def step(gauge, momenta):
        shape = gauge.shape
        flat = (4, 18) + shape[4:]
        field = jax.ShapeDtypeStruct(flat, F32)
        dma = pltpu.SemaphoreType.DMA
        any_space = pl.BlockSpec(memory_space=pl.ANY)
        links, final, plaquette = pl.pallas_call(
            lambda *refs: kernel(sizes, *refs),
            name="md_step",
            out_shape=(field, field, jax.ShapeDtypeStruct((1, 1), F32)),
            in_specs=[any_space] * 2,
            out_specs=(any_space, any_space, pl.BlockSpec(memory_space=pltpu.SMEM)),
            scratch_shapes=[
                pltpu.VMEM((2, 4, 18, 2, 8, 128), F32),
                pltpu.VMEM((2, 4, 4, 18, 2, 8, 128), F32),
                pltpu.VMEM((2, 3, 18, 2, 1, 128), F32),
                pltpu.VMEM((2, 3, 18, 2, 1, 128), F32),
                pltpu.VMEM((2, 3, 18, 8, 128), F32),
                pltpu.VMEM((2, 3, 18, 8, 128), F32),
                pltpu.VMEM((4, 4, 8, 2, 8, 128), F32),
                pltpu.VMEM((2, 4, 4, 8, 3, 8, 128), F32),
                pltpu.VMEM((2, 3, 8, 2, 1, 128), F32),
                pltpu.VMEM((2, 3, 8, 2, 1, 128), F32),
                pltpu.VMEM((2, 3, 8, 8, 128), F32),
                pltpu.VMEM((2, 3, 8, 8, 128), F32),
                pltpu.VMEM((4, 18, 2, 8, 128), F32),
                pltpu.VMEM((4, 18, 2, 8, 128), F32),
                pltpu.VMEM((12, 8, 128), F32),
                pltpu.VMEM((3, max(sizes), 1, 128), F32),
                dma((8,)),
                dma((2, 4)), dma((2, 4)), dma((2,)), dma((2,)), dma((2, 3)), dma((2, 3)),
                dma((2, 4)), dma((2, 4)), dma((2,)), dma((2,)), dma((2, 3)), dma((2, 3)),
                dma((3, max(sizes))), dma((3, max(sizes))), dma((2,)),
            ],
            compiler_params=pltpu.CompilerParams(collective_id=0, has_side_effects=True, vmem_limit_bytes=48 * 1024 * 1024),
        )(gauge.reshape(flat), momenta.reshape(flat))
        return links.reshape(shape), final.reshape(shape), plaquette[0, 0]

    return jax.shard_map(step, mesh=mesh, in_specs=(spec, spec), out_specs=(spec, spec, P()), check_vma=False)
```

```python
import jax
import jax.numpy as jnp
from jax import lax
from jax.experimental import pallas as pl
from jax.experimental.pallas import tpu as pltpu
from jax.sharding import PartitionSpec as P

MESH = pl.DeviceIdType.MESH
F32 = jnp.float32
KICK = 0.25
STEP = 0.2
NAMES = ("gx", "gy", "zt")
LEAD = {(0, 1): 1, (0, 2): 2, (0, 3): 3, (1, 2): 2, (1, 3): 1, (2, 3): 3}


def load_matrix(ref, lead, *rest):
    return [[(ref[(*lead, 3 * i + j, *rest)], ref[(*lead, 9 + 3 * i + j, *rest)]) for j in range(3)] for i in range(3)]


def store_matrix(ref, lead, rest, value):
    for i in range(3):
        for j in range(3):
            for part in range(2):
                ref[(*lead, 9 * part + 3 * i + j, *rest)] = value[i][j][part]


def add(a, b):
    return b if a is None else a + b


def product(a, b):
    out = []
    for i in range(3):
        line = []
        for j in range(3):
            re, im = None, None
            for k in range(3):
                ar, ai = a[i][k]
                br, bi = b[k][j]
                re = add(re, ar * br - ai * bi)
                im = add(im, ar * bi + ai * br)
            line.append((re, im))
        out.append(line)
    return out


def dagger(a):
    return [[(a[j][i][0], -a[j][i][1]) for j in range(3)] for i in range(3)]


def dagger_product(a, b):
    out = []
    for i in range(3):
        line = []
        for j in range(3):
            re, im = None, None
            for k in range(3):
                ar, ai = a[k][i]
                br, bi = b[k][j]
                re = add(re, ar * br + ai * bi)
                im = add(im, ar * bi - ai * br)
            line.append((re, im))
        out.append(line)
    return out


def dagger_entry(x, y, i, j):
    re, im = None, None
    for k in range(3):
        ar, ai = x[i][k]
        br, bi = y[j][k]
        re = add(re, ar * br + ai * bi)
        im = add(im, ai * br - ar * bi)
    return re, im


def twice_traceless(x, y):
    diag = []
    for i in range(3):
        im = None
        for k in range(3):
            ar, ai = x[i][k]
            br, bi = y[i][k]
            im = add(im, ai * br - ar * bi)
        diag.append(im)
    mean = (diag[0] + diag[1] + diag[2]) * (2.0 / 3.0)
    out = [diag[0] + diag[0] - mean, diag[1] + diag[1] - mean]
    for i, j in ((0, 1), (0, 2), (1, 2)):
        pr, pi = dagger_entry(x, y, i, j)
        qr, qi = dagger_entry(x, y, j, i)
        out += [pr - qr, pi + qi]
    return out


def real_trace(x, y):
    total = None
    for i in range(3):
        for k in range(3):
            ar, ai = x[i][k]
            br, bi = y[i][k]
            total = add(total, ar * br + ai * bi)
    return total


def conjugated(d, t):
    d0, d1, ur, ui, vr, vi, wr, wi = t
    d2 = -(d0 + d1)

    def column(j):
        (ar, ai), (br, bi), (cr, ci) = d[0][j], d[1][j], d[2][j]
        first = (
            ur * br - ui * bi + (vr * cr - vi * ci) - d0 * ai,
            ur * bi + ui * br + (vr * ci + vi * cr) + d0 * ar,
        )
        second = (
            wr * cr - wi * ci - (ur * ar + ui * ai) - d1 * bi,
            wr * ci + wi * cr + (ui * ar - ur * ai) + d1 * br,
        )
        third = (
            -(vr * ar + vi * ai) - (wr * br + wi * bi) - d2 * ci,
            (vi * ar - vr * ai) + (wi * br - wr * bi) + d2 * cr,
        )
        return first, second, third

    def imag(i, col):
        total = None
        for k in range(3):
            ar, ai = d[k][i]
            total = add(total, ar * col[k][1] - ai * col[k][0])
        return total

    def entry(i, col):
        re, im = None, None
        for k in range(3):
            ar, ai = d[k][i]
            br, bi = col[k]
            re = add(re, ar * br + ai * bi)
            im = add(im, ar * bi - ai * br)
        return re, im

    zero = column(0)
    e0 = imag(0, zero)
    one = column(1)
    e1 = imag(1, one)
    u = entry(0, one)
    two = column(2)
    v = entry(0, two)
    w = entry(1, two)
    return [e0, e1, u[0], u[1], v[0], v[1], w[0], w[1]]


def cayley(h, scale):
    a0, a1, ur, ui, vr, vi, wr, wi = [scale * part for part in h]
    a2 = -(a0 + a1)
    uu = ur * ur + ui * ui
    vv = vr * vr + vi * vi
    ww = wr * wr + wi * wi
    s00, s11, s22 = a0 * a0, a1 * a1, a2 * a2
    one_s = 1.0 + (0.5 * (s00 + s11 + s22) + (uu + vv + ww))
    uwr, uwi = ur * wr - ui * wi, ur * wi + ui * wr
    det_h = a0 * a1 * a2 + 2.0 * (uwi * vr - uwr * vi) - a0 * ww - a1 * vv - a2 * uu
    scale2 = 2.0 / (one_s * one_s + det_h * det_h)
    qr, qi = one_s * scale2, -(det_h * scale2)
    pr, pi = a2 * ui - (vr * wr + vi * wi), -(a2 * ur) - (vi * wr - vr * wi)
    rr, ri = a1 * vi + uwr, uwi - a1 * vr
    tr, ti = a0 * wi - (ur * vr + ui * vi), -(a0 * wr) - (ur * vi - ui * vr)
    rows = [
        [(one_s - (s00 + uu + vv), a0), (ur + pr, ui + pi), (vr + rr, vi + ri)],
        [(pr - ur, ui - pi), (one_s - (s11 + uu + ww), a1), (wr + tr, wi + ti)],
        [(rr - vr, vi - ri), (tr - wr, wi - ti), (one_s - (s22 + vv + ww), a2)],
    ]
    out = []
    for i in range(3):
        line = []
        for j in range(3):
            br, bi = rows[i][j]
            re, im = br * qr - bi * qi, br * qi + bi * qr
            line.append((re - 1.0 if i == j else re, im))
        out.append(line)
    return out


PARTS = (9, 13, 1, 10, 2, 11, 5, 14)
ROWS = (0, 2, 3)


def kernel(
    sizes, gauge, momenta, new_links, final, plaquette,
    old_links, moment, time_ahead, row_ahead, lane_ahead, mixed,
    loops, lower, lower_time,
    row_out, row_in, x_in, lane_out, lane_in, mix_out, mix_in,
    low_row_out, low_row_in, low_lane_out, low_lane_in, time_out, time_in,
    traces, gather_z, gather_rest,
    load_sem, send_sem, recv_sem, z_send, z_recv, rest_send, rest_recv, known_sem,
):
    me = [lax.axis_index(name) for name in NAMES]
    links = (old_links, new_links)
    half = sizes[2] // 2
    my_half, my_z = me[2] // half, lax.rem(me[2], half)

    def peer(axis, offset):
        return {NAMES[axis]: lax.rem(me[axis] + (offset + sizes[axis]), sizes[axis])}

    def z_peer(offset):
        return {"zt": my_half * half + lax.rem(my_z + offset, half)}

    rest = [(i, j, k) for i in range(sizes[0]) for j in range(sizes[1]) for k in range(2) if i + j + k]

    def rest_peer(offset):
        i, j, k = offset
        return {**peer(0, i), **peer(1, j), "zt": lax.rem(my_half + k, 2) * half + my_z}

    barrier = pltpu.get_barrier_semaphore()
    neighbours = [peer(axis, offset) for axis in range(3) for offset in (-1, 1)]
    for device in neighbours:
        pl.semaphore_signal(barrier, inc=1, device_id=device, device_id_type=MESH)

    loads = {m: pltpu.make_async_copy(gauge.at[m], old_links.at[m], load_sem.at[m]) for m in (1, 0, 2, 3)}
    loads[4] = pltpu.make_async_copy(momenta, moment, load_sem.at[4])
    for copy in loads.values():
        copy.start()

    def known(step, *offsets):
        for offset in offsets:
            pl.semaphore_signal(known_sem.at[step], inc=1, device_id=peer(2, offset), device_id_type=MESH)

    lane = lax.broadcasted_iota(jnp.int32, (8, 128), 1)
    row = lax.broadcasted_iota(jnp.int32, (8, 128), 0)
    low = lane < 64
    time = lax.rem(lane, 64)
    last_time = time == 63
    first_time = time == 0
    last_row = row == 7
    first_row = row == 0

    def flip(value):
        return pltpu.roll(value, 64, 1)

    def remote(ph, name):
        now = links[ph]
        number, src, dst, axis, offset = {
            "x1": (0, now.at[1, :, 0], x_in.at[ph, 0], 0, -1),
            "x2": (1, now.at[2, :, 0], x_in.at[ph, 1], 0, -1),
            "y": (2, row_out.at[ph], row_in.at[ph], 1, -1),
            "z0": (3, lane_out.at[ph, 0], lane_in.at[ph, 0], 2, -1),
            "z1": (4, lane_out.at[ph, 1], lane_in.at[ph, 1], 2, -1),
            "mx": (5, mixed.at[ph, 0, :, 2], mixed.at[ph, 0, :, 0], 0, 1),
            "mz": (6, mix_out.at[ph], mix_in.at[ph], 2, 1),
            "lx1": (7, lower.at[ph, 0, 1, :, 2], lower.at[ph, 0, 1, :, 0], 0, 1),
            "lx2": (8, lower.at[ph, 0, 2, :, 2], lower.at[ph, 0, 2, :, 0], 0, 1),
            "ly": (9, low_row_out.at[ph], low_row_in.at[ph], 1, 1),
            "lz0": (10, low_lane_out.at[ph, 0], low_lane_in.at[ph, 0], 2, 1),
            "lz1": (11, low_lane_out.at[ph, 1], low_lane_in.at[ph, 1], 2, 1),
            "tx": (12, lower.at[ph, 0, 3, :, 0], lower.at[ph, 0, 3, :, 2], 0, -1),
            "tz": (13, time_out.at[ph], time_in.at[ph], 2, -1),
        }[name]
        return pltpu.make_async_remote_copy(
            src_ref=src, dst_ref=dst, send_sem=send_sem.at[ph, number], recv_sem=recv_sem.at[ph, number],
            device_id=peer(axis, offset), device_id_type=MESH)

    names = ("x1", "x2", "y", "z0", "z1", "mx", "mz", "lx1", "lx2", "ly", "lz0", "lz1", "tx", "tz")

    def z_sum(offset):
        return pltpu.make_async_remote_copy(
            src_ref=gather_z.at[my_z], dst_ref=gather_z.at[my_z],
            send_sem=z_send.at[offset], recv_sem=z_recv.at[offset],
            device_id=z_peer(offset), device_id_type=MESH)

    my_rest = (me[0] * sizes[1] + me[1]) * 2 + my_half

    def rest_sum(offset):
        number = (offset[0] * sizes[1] + offset[1]) * 2 + offset[2]
        return pltpu.make_async_remote_copy(
            src_ref=gather_rest.at[my_rest], dst_ref=gather_rest.at[my_rest],
            send_sem=rest_send.at[number], recv_sem=rest_recv.at[number],
            device_id=rest_peer(offset), device_id_type=MESH)

    def loop(count, body):
        def step(i, _):
            body(i)
            return 0
        lax.fori_loop(0, count, step, 0)

    def plane(ph, m, n, x, b, c, slot, split=False):
        a = load_matrix(links[ph], (m,), x)
        left = product(a, b)
        d = load_matrix(links[ph], (n,), x)
        right = product(d, c)
        t = twice_traceless(left, right)
        if ph == 1:
            traces[slot] = real_trace(left, right)
        for p in range(8):
            loops[m, n, p, x] = t[p]
        if not split:
            below(ph, m, n, x, a, d, t)

    def below(ph, m, n, x, a, d, t):
        for p, value in enumerate(conjugated(d, t)):
            lower[ph, n, m, p, x + 1] = value
        for p, value in enumerate(conjugated(a, t)):
            lower[ph, m, n, p, x + 1] = value

    def ahead_x(ph, n, x):
        return load_matrix(links[ph], (n,), 1) if x == 0 else load_matrix(x_in, (ph, n - 1))

    def pack_lanes(ph, m):
        for c in range(18):
            v0 = links[ph][m, c, 0]
            v1 = links[ph][m, c, 1]
            r0 = flip(v0)
            lane_out[ph, m, c] = jnp.where(low, v1, r0)
            lane_ahead[m, c, 0] = r0
            lane_ahead[m, c, 1] = flip(v1)

    def send_edges(ph, m):
        if m in (0, 1):
            remote(ph, "z" + str(m)).start()
        if m in (1, 2):
            remote(ph, "x" + str(m)).start()

    def first_half(ph):
        def shift_time(n, x):
            for c in range(18):
                v = links[ph][n, c, x]
                time_ahead[n, c, x] = jnp.where(last_time, pltpu.roll(v, 63, 1), pltpu.roll(v, 127, 1))

        def mix(d, x):
            left = product(load_matrix(links[ph], (3,), x), load_matrix(time_ahead, (d,), x))
            store_matrix(mixed, (ph, d // 2), (x + 1,), dagger_product(load_matrix(links[ph], (d,), x), left))

        loop(2, lambda x: shift_time(2, x))
        loop(2, lambda x: mix(2, x))
        for c in range(18):
            mix_out[ph, c] = jnp.where(low, flip(mixed[ph, 1, c, 1]), mixed[ph, 1, c, 2])
        remote(ph, "mz").start()

        def pack_rows(x):
            for k, n in enumerate(ROWS):
                for c in range(18):
                    row_out[ph, k, c, x] = links[ph][n, c, x, 0:1, :]
        loop(2, pack_rows)
        remote(ph, "y").start()

        loop(4, lambda i: shift_time(i // 2, lax.rem(i, 2)))
        loop(2, lambda x: mix(0, x))
        remote(ph, "mx").start()

        remote(ph, "y").wait_recv()

        def shift_rows(i):
            k, x = i // 2, lax.rem(i, 2)
            n = k + (k + 1) // 2
            for c in range(18):
                v = links[ph][n, c, x]
                edge = jnp.broadcast_to(row_in[ph, k, c, x], (8, 128))
                row_ahead[n, c, x] = jnp.where(last_row, edge, pltpu.roll(v, 7, 0))
        loop(6, shift_rows)

        plane(ph, 1, 0, 0, load_matrix(row_ahead, (0,), 0), ahead_x(ph, 1, 0), 0)
        loop(2, lambda x: plane(
            ph, 1, 3, x, load_matrix(row_ahead, (3,), x), load_matrix(time_ahead, (1,), x), 2 + x))

        remote(ph, "x1").wait_recv()
        plane(ph, 1, 0, 1, load_matrix(row_ahead, (0,), 1), ahead_x(ph, 1, 1), 1)
        remote(ph, "lx1").start()

        def ahead_z(m):
            for c in range(18):
                edge = lane_in[ph, m, c]
                lane_ahead[m, c, 0] = jnp.where(low, lane_ahead[m, c, 0], edge)
                lane_ahead[m, c, 1] = jnp.where(low, lane_ahead[m, c, 1], flip(edge))

        def pack_lower(m):
            for p in range(8):
                low_lane_out[ph, m, p] = jnp.where(low, flip(lower[ph, 2, m, p, 1]), lower[ph, 2, m, p, 2])

        remote(ph, "z1").wait_recv()
        ahead_z(1)
        loop(2, lambda x: plane(
            ph, 2, 1, x, load_matrix(lane_ahead, (1,), x), load_matrix(row_ahead, (2,), x), 4 + x))
        pack_lower(1)
        remote(ph, "lz1").start()
        for k, m in enumerate(ROWS):
            for p in range(8):
                for x in range(2):
                    low_row_out[ph, k, p, x] = lower[ph, 1, m, p, x + 1, 7:8, :]
        remote(ph, "ly").start()

        remote(ph, "mx").wait_recv()
        def seen_x(x):
            m, c = load_matrix(mixed, (ph, 0), x), load_matrix(links[ph], (3,), x)
            if ph == 1:
                traces[6 + x] = real_trace(m, c)
            for p, value in enumerate(twice_traceless(m, c)):
                lower[ph, 0, 3, p, x] = value
        loop(2, seen_x)
        remote(ph, "tx").start()
        remote(ph, "mz").wait_recv()
        for c in range(18):
            edge = mix_in[ph, c]
            mixed[ph, 1, c, 0] = jnp.where(low, edge, flip(mixed[ph, 1, c, 1]))
            mixed[ph, 1, c, 1] = jnp.where(low, flip(edge), flip(mixed[ph, 1, c, 2]))
        def seen_z(x):
            m, c = load_matrix(mixed, (ph, 1), x), load_matrix(links[ph], (3,), x)
            if ph == 1:
                traces[8 + x] = real_trace(m, c)
            for p, value in enumerate(twice_traceless(m, c)):
                lower_time[p, x] = value
        loop(2, seen_z)
        for p in range(8):
            time_out[ph, p] = jnp.where(low, lower_time[p, 1], flip(lower_time[p, 0]))
        remote(ph, "tz").start()

        remote(ph, "x2").wait_recv()
        remote(ph, "z0").wait_recv()
        ahead_z(0)
        for x in (1, 0):
            plane(ph, 2, 0, x, load_matrix(lane_ahead, (0,), x), ahead_x(ph, 2, x), 10 + x, split=ph == 1)
            if ph == 0 and x == 1:
                remote(ph, "lx2").start()
        if ph == 0:
            known(0, -2, 2)
        else:
            total = traces[0]
            for slot in range(1, 12):
                total = total + traces[slot]
            gather_z[my_z] = jnp.sum(total, axis=0, keepdims=True)
            pl.semaphore_wait(known_sem.at[1], 2)
            for offset in range(1, half):
                z_sum(offset).start()
            known(2, half)
            for x in (1, 0):
                below(ph, 2, 0, x, load_matrix(links[ph], (2,), x), load_matrix(links[ph], (0,), x),
                      [loops[2, 0, p, x] for p in range(8)])
                if x == 1:
                    remote(ph, "lx2").start()
        pack_lower(0)
        remote(ph, "lz0").start()

        def own(n, x, seen):
            t = conjugated(dagger(load_matrix(links[ph], (n,), x)), seen)
            for p in range(8):
                loops[3, n, p, x] = t[p]
            for p, value in enumerate(conjugated(load_matrix(links[ph], (3,), x), t)):
                lower[ph, 3, n, p, x + 1] = value
        remote(ph, "tx").wait_recv()
        loop(2, lambda x: own(0, x, [lower[ph, 0, 3, p, x + 1] for p in range(8)]))
        if ph == 1:
            for offset in range(1, half):
                z_sum(offset).wait_recv()
            total = gather_z[0]
            for source in range(1, half):
                total = total + gather_z[source]
            gather_rest[my_rest] = total
            pl.semaphore_wait(known_sem.at[2], 1)
            for offset in rest:
                rest_sum(offset).start()
        remote(ph, "tz").wait_recv()
        loop(2, lambda x: own(2, x, [
            jnp.where(low, flip(lower_time[p, x]), pltpu.roll(time_in[ph, p], 64 * x, 1)) for p in range(8)]))

        for name in ("ly", "lx1", "lz1", "lx2", "lz0"):
            remote(ph, name).wait_recv()
        if ph == 0:
            pl.semaphore_wait(known_sem.at[0], 2)
            known(1, -4, 4)

    def half_step(ph, m, x):
        total = [None] * 8
        for n in range(4):
            if n == m:
                continue
            lead = LEAD[min(m, n), max(m, n)]
            first, second = (m, n) if lead == m else (n, m)
            for p in range(8):
                here = loops[first, second, p, x]
                if n == 0:
                    below = lower[ph, 0, m, p, x]
                elif n == 1:
                    edge = jnp.broadcast_to(low_row_in[ph, ROWS.index(m), p, x], (8, 128))
                    below = jnp.where(first_row, edge, pltpu.roll(lower[ph, 1, m, p, x + 1], 1, 0))
                elif n == 2 and m == 3:
                    below = lower_time[p, x]
                elif n == 2:
                    edge = pltpu.roll(low_lane_in[ph, m, p], 64 * x, 1)
                    below = jnp.where(low, edge, flip(lower[ph, 2, m, p, x + 1]))
                else:
                    value = lower[ph, 3, m, p, x + 1]
                    below = jnp.where(first_time, pltpu.roll(value, 65, 1), pltpu.roll(value, 1, 1))
                total[p] = add(total[p], here - below if lead == m else below - here)
        return [moment[m, PARTS[p], x] - (0.5 * KICK) * total[p] for p in range(8)]

    for m in (1, 0):
        loads[m].wait()
        pack_lanes(0, m)
    pl.semaphore_wait(barrier, len(neighbours))
    send_edges(0, 1)
    send_edges(0, 0)
    loads[2].wait()
    send_edges(0, 2)
    loads[3].wait()
    first_half(0)
    loads[4].wait()
    for m in (1, 0, 2, 3):
        def update(x):
            h = half_step(0, m, x)
            for p in range(8):
                moment[m, PARTS[p], x] = h[p]
            u = cayley(h, 0.5 * STEP)
            store_matrix(new_links, (m,), (x,), product(u, load_matrix(old_links, (m,), x)))
        loop(2, update)
        if m in (0, 1):
            pack_lanes(1, m)
        send_edges(1, m)
    first_half(1)

    def finish(x):
        for m in range(4):
            h = half_step(1, m, x)
            for p in range(8):
                final[m, PARTS[p], x] = h[p]
            final[m, 17, x] = -(h[0] + h[1])
            for c, p in ((3, 2), (6, 4), (7, 6)):
                final[m, c, x] = -h[p]
                final[m, 9 + c, x] = h[p + 1]
            for c in (0, 4, 8):
                final[m, c, x] = jnp.zeros((8, 128), F32)
    loop(2, finish)

    for ph in range(2):
        for name in names:
            remote(ph, name).wait_send()
    for offset in range(1, half):
        z_sum(offset).wait_send()
    for offset in rest:
        rest_sum(offset).wait_send()
    for offset in rest:
        rest_sum(offset).wait_recv()
    total = gather_rest[0]
    for source in range(1, len(rest) + 1):
        total = total + gather_rest[source]
    volume = 72.0 * (2 * 8 * 128) * (sizes[0] * sizes[1] * sizes[2])
    plaquette[0, 0] = jnp.sum(total) * (4.0 / volume)


def solution(mesh):
    sizes = tuple(mesh.shape[name] for name in NAMES)
    spec = P(None, None, None, None, "gx", "gy", "zt")

    def step(gauge, momenta):
        shape = gauge.shape
        flat = (4, 18) + shape[4:]
        field = jax.ShapeDtypeStruct(flat, F32)
        dma = pltpu.SemaphoreType.DMA
        vmem = pl.BlockSpec(memory_space=pltpu.VMEM)
        half = sizes[2] // 2
        others = sizes[0] * sizes[1] * 2
        tile = (8, 128)

        def scratch(*lead):
            return pltpu.VMEM(lead + tile, F32)

        def rows(*lead):
            return pltpu.VMEM(lead + (1, 128), F32)

        links, final, plaquette = pl.pallas_call(
            lambda *refs: kernel(sizes, *refs),
            name="md_step",
            out_shape=(field, field, jax.ShapeDtypeStruct((1, 1), F32)),
            in_specs=[pl.BlockSpec(memory_space=pltpu.HBM)] * 2,
            out_specs=(vmem, vmem, pl.BlockSpec(memory_space=pltpu.SMEM)),
            scratch_shapes=[
                scratch(4, 18, 2), scratch(4, 18, 2), scratch(3, 18, 2), scratch(4, 18, 2), scratch(2, 18, 2),
                scratch(2, 2, 18, 3),
                scratch(4, 4, 8, 2), scratch(2, 4, 4, 8, 3), scratch(8, 2),
                rows(2, 3, 18, 2), rows(2, 3, 18, 2), scratch(2, 2, 18), scratch(2, 2, 18), scratch(2, 2, 18),
                scratch(2, 18), scratch(2, 18),
                rows(2, 3, 8, 2), rows(2, 3, 8, 2), scratch(2, 2, 8), scratch(2, 2, 8), scratch(2, 8), scratch(2, 8),
                scratch(12), rows(half), rows(others),
                dma((5,)), dma((2, 14)), dma((2, 14)), dma((half,)), dma((half,)), dma((others,)), dma((others,)),
                pltpu.SemaphoreType.REGULAR((3,)),
            ],
            compiler_params=pltpu.CompilerParams(collective_id=0, has_side_effects=True, vmem_limit_bytes=48 * 1024 * 1024),
        )(*(pltpu.with_memory_space_constraint(a.reshape(flat), pltpu.HBM) for a in (gauge, momenta)))
        return links.reshape(shape), final.reshape(shape), plaquette[0, 0]

    return jax.shard_map(step, mesh=mesh, in_specs=(spec, spec), out_specs=(spec, spec, P()), check_vma=False)
```

```python
import jax
import jax.numpy as jnp
from jax import lax
from jax.experimental import pallas as pl
from jax.experimental.pallas import tpu as pltpu
from jax.sharding import PartitionSpec as P

MESH = pl.DeviceIdType.MESH
F32 = jnp.float32
KICK = 0.25
STEP = 0.2
NAMES = ("gx", "gy", "zt")
LEAD = {(0, 1): 1, (0, 2): 2, (0, 3): 3, (1, 2): 2, (1, 3): 1, (2, 3): 3}


def load_matrix(ref, lead, *rest):
    return [[(ref[(*lead, 3 * i + j, *rest)], ref[(*lead, 9 + 3 * i + j, *rest)]) for j in range(3)] for i in range(3)]


def store_matrix(ref, lead, rest, value):
    for i in range(3):
        for j in range(3):
            for part in range(2):
                ref[(*lead, 9 * part + 3 * i + j, *rest)] = value[i][j][part]


def add(a, b):
    return b if a is None else a + b


def product(a, b):
    out = []
    for i in range(3):
        line = []
        for j in range(3):
            re, im = None, None
            for k in range(3):
                ar, ai = a[i][k]
                br, bi = b[k][j]
                re = add(re, ar * br - ai * bi)
                im = add(im, ar * bi + ai * br)
            line.append((re, im))
        out.append(line)
    return out


def dagger(a):
    return [[(a[j][i][0], -a[j][i][1]) for j in range(3)] for i in range(3)]


def dagger_product(a, b):
    out = []
    for i in range(3):
        line = []
        for j in range(3):
            re, im = None, None
            for k in range(3):
                ar, ai = a[k][i]
                br, bi = b[k][j]
                re = add(re, ar * br + ai * bi)
                im = add(im, ar * bi - ai * br)
            line.append((re, im))
        out.append(line)
    return out


def dagger_entry(x, y, i, j):
    re, im = None, None
    for k in range(3):
        ar, ai = x[i][k]
        br, bi = y[j][k]
        re = add(re, ar * br + ai * bi)
        im = add(im, ai * br - ar * bi)
    return re, im


def twice_traceless(x, y):
    diag = []
    for i in range(3):
        im = None
        for k in range(3):
            ar, ai = x[i][k]
            br, bi = y[i][k]
            im = add(im, ai * br - ar * bi)
        diag.append(im)
    mean = (diag[0] + diag[1] + diag[2]) * (2.0 / 3.0)
    out = [diag[0] + diag[0] - mean, diag[1] + diag[1] - mean]
    for i, j in ((0, 1), (0, 2), (1, 2)):
        pr, pi = dagger_entry(x, y, i, j)
        qr, qi = dagger_entry(x, y, j, i)
        out += [pr - qr, pi + qi]
    return out


def real_trace(x, y):
    total = None
    for i in range(3):
        for k in range(3):
            ar, ai = x[i][k]
            br, bi = y[i][k]
            total = add(total, ar * br + ai * bi)
    return total


def conjugated(d, t):
    d0, d1, ur, ui, vr, vi, wr, wi = t
    d2 = -(d0 + d1)

    def column(j):
        (ar, ai), (br, bi), (cr, ci) = d[0][j], d[1][j], d[2][j]
        first = (
            ur * br - ui * bi + (vr * cr - vi * ci) - d0 * ai,
            ur * bi + ui * br + (vr * ci + vi * cr) + d0 * ar,
        )
        second = (
            wr * cr - wi * ci - (ur * ar + ui * ai) - d1 * bi,
            wr * ci + wi * cr + (ui * ar - ur * ai) + d1 * br,
        )
        third = (
            -(vr * ar + vi * ai) - (wr * br + wi * bi) - d2 * ci,
            (vi * ar - vr * ai) + (wi * br - wr * bi) + d2 * cr,
        )
        return first, second, third

    def imag(i, col):
        total = None
        for k in range(3):
            ar, ai = d[k][i]
            total = add(total, ar * col[k][1] - ai * col[k][0])
        return total

    def entry(i, col):
        re, im = None, None
        for k in range(3):
            ar, ai = d[k][i]
            br, bi = col[k]
            re = add(re, ar * br + ai * bi)
            im = add(im, ar * bi - ai * br)
        return re, im

    zero = column(0)
    e0 = imag(0, zero)
    one = column(1)
    e1 = imag(1, one)
    u = entry(0, one)
    two = column(2)
    v = entry(0, two)
    w = entry(1, two)
    return [e0, e1, u[0], u[1], v[0], v[1], w[0], w[1]]


def cayley(h, scale):
    a0, a1, ur, ui, vr, vi, wr, wi = [scale * part for part in h]
    a2 = -(a0 + a1)
    uu = ur * ur + ui * ui
    vv = vr * vr + vi * vi
    ww = wr * wr + wi * wi
    s00, s11, s22 = a0 * a0, a1 * a1, a2 * a2
    one_s = 1.0 + (0.5 * (s00 + s11 + s22) + (uu + vv + ww))
    uwr, uwi = ur * wr - ui * wi, ur * wi + ui * wr
    det_h = a0 * a1 * a2 + 2.0 * (uwi * vr - uwr * vi) - a0 * ww - a1 * vv - a2 * uu
    scale2 = 2.0 / (one_s * one_s + det_h * det_h)
    qr, qi = one_s * scale2, -(det_h * scale2)
    pr, pi = a2 * ui - (vr * wr + vi * wi), -(a2 * ur) - (vi * wr - vr * wi)
    rr, ri = a1 * vi + uwr, uwi - a1 * vr
    tr, ti = a0 * wi - (ur * vr + ui * vi), -(a0 * wr) - (ur * vi - ui * vr)
    rows = [
        [(one_s - (s00 + uu + vv), a0), (ur + pr, ui + pi), (vr + rr, vi + ri)],
        [(pr - ur, ui - pi), (one_s - (s11 + uu + ww), a1), (wr + tr, wi + ti)],
        [(rr - vr, vi - ri), (tr - wr, wi - ti), (one_s - (s22 + vv + ww), a2)],
    ]
    out = []
    for i in range(3):
        line = []
        for j in range(3):
            br, bi = rows[i][j]
            re, im = br * qr - bi * qi, br * qi + bi * qr
            line.append((re - 1.0 if i == j else re, im))
        out.append(line)
    return out


PARTS = (9, 13, 1, 10, 2, 11, 5, 14)
ROWS = (0, 2, 3)
LANES = (0, 1, 3)


def kernel(
    sizes, gauge, momenta, new_links, final, plaquette,
    old_links, moment, time_ahead, row_ahead, lane_ahead, mixed_x, mixed_z,
    loops, lower, lower_z,
    row_out, row_in, x_in, lane_out, lane_in, mix_out, mix_in,
    low_row_out, low_row_in,
    traces, gather_z, gather_rest,
    load_sem, send_sem, recv_sem, z_send, z_recv, rest_send, rest_recv, known_sem,
):
    me = [lax.axis_index(name) for name in NAMES]
    links = (old_links, new_links)
    half = sizes[2] // 2
    my_half, my_z = me[2] // half, lax.rem(me[2], half)

    def peer(axis, offset):
        return {NAMES[axis]: lax.rem(me[axis] + (offset + sizes[axis]), sizes[axis])}

    def z_peer(offset):
        return {"zt": my_half * half + lax.rem(my_z + offset, half)}

    rest = [(i, j, k) for i in range(sizes[0]) for j in range(sizes[1]) for k in range(2) if i + j + k]

    def rest_peer(offset):
        i, j, k = offset
        return {**peer(0, i), **peer(1, j), "zt": lax.rem(my_half + k, 2) * half + my_z}

    barrier = pltpu.get_barrier_semaphore()
    neighbours = [peer(axis, offset) for axis in range(3) for offset in (-1, 1)]
    for device in neighbours:
        pl.semaphore_signal(barrier, inc=1, device_id=device, device_id_type=MESH)

    loads = {m: pltpu.make_async_copy(gauge.at[m], old_links.at[m], load_sem.at[m]) for m in (2, 0, 1, 3)}
    for copy in loads.values():
        copy.start()
    loads[4] = pltpu.make_async_copy(momenta, moment, load_sem.at[4])

    def known(step, *offsets):
        for offset in offsets:
            pl.semaphore_signal(known_sem.at[step], inc=1, device_id=peer(2, offset), device_id_type=MESH)

    lane = lax.broadcasted_iota(jnp.int32, (8, 128), 1)
    row = lax.broadcasted_iota(jnp.int32, (8, 128), 0)
    low = lane < 64
    time = lax.rem(lane, 64)
    last_time = time == 63
    first_time = time == 0
    last_row = row == 7
    first_row = row == 0

    def flip(value):
        return pltpu.roll(value, 64, 1)

    def remote(ph, name):
        now = links[ph]
        number, src, dst, axis, offset = {
            "x1": (0, now.at[1, :, 0], x_in.at[ph, 0], 0, -1),
            "x2": (1, now.at[2, :, 0], x_in.at[ph, 1], 0, -1),
            "y": (2, row_out.at[ph], row_in.at[ph], 1, -1),
            "z0": (3, lane_out.at[ph, 0], lane_in.at[ph, 0], 2, -1),
            "z1": (4, lane_out.at[ph, 1], lane_in.at[ph, 1], 2, -1),
            "z3": (5, lane_out.at[ph, 2], lane_in.at[ph, 2], 2, -1),
            "mx": (6, mixed_x.at[ph, :, 2], mixed_x.at[ph, :, 0], 0, 1),
            "mz0": (7, mix_out.at[ph, 0], mix_in.at[ph, 0], 2, 1),
            "mz1": (8, mix_out.at[ph, 1], mix_in.at[ph, 1], 2, 1),
            "mz3": (9, mix_out.at[ph, 2], mix_in.at[ph, 2], 2, 1),
            "lx1": (10, lower.at[ph, 0, 1, :, 2], lower.at[ph, 0, 1, :, 0], 0, 1),
            "lx2": (11, lower.at[ph, 0, 2, :, 2], lower.at[ph, 0, 2, :, 0], 0, 1),
            "ly": (12, low_row_out.at[ph], low_row_in.at[ph], 1, 1),
            "tx": (13, lower.at[ph, 0, 3, :, 0], lower.at[ph, 0, 3, :, 2], 0, -1),
        }[name]
        return pltpu.make_async_remote_copy(
            src_ref=src, dst_ref=dst, send_sem=send_sem.at[ph, number], recv_sem=recv_sem.at[ph, number],
            device_id=peer(axis, offset), device_id_type=MESH)

    names = ("x1", "x2", "y", "z0", "z1", "z3", "mx", "mz0", "mz1", "mz3", "lx1", "lx2", "ly", "tx")

    def z_sum(offset):
        return pltpu.make_async_remote_copy(
            src_ref=gather_z.at[my_z], dst_ref=gather_z.at[my_z],
            send_sem=z_send.at[offset], recv_sem=z_recv.at[offset],
            device_id=z_peer(offset), device_id_type=MESH)

    my_rest = (me[0] * sizes[1] + me[1]) * 2 + my_half

    def rest_sum(offset):
        number = (offset[0] * sizes[1] + offset[1]) * 2 + offset[2]
        return pltpu.make_async_remote_copy(
            src_ref=gather_rest.at[my_rest], dst_ref=gather_rest.at[my_rest],
            send_sem=rest_send.at[number], recv_sem=rest_recv.at[number],
            device_id=rest_peer(offset), device_id_type=MESH)

    def loop(count, body):
        def step(i, _):
            body(i)
            return 0
        lax.fori_loop(0, count, step, 0)

    def plane(ph, m, n, x, b, c, slot, split=False):
        a = load_matrix(links[ph], (m,), x)
        left = product(a, b)
        d = load_matrix(links[ph], (n,), x)
        right = product(d, c)
        t = twice_traceless(left, right)
        if ph == 1 and slot is not None:
            traces[slot] = real_trace(left, right)
        for p in range(8):
            loops[m, n, p, x] = t[p]
        if not split:
            below(ph, m, n, x, t)

    def below(ph, m, n, x, t):
        if n != 2:
            for p, value in enumerate(conjugated(load_matrix(links[ph], (n,), x), t)):
                lower[ph, n, m, p, x + 1] = value
        if m != 2:
            for p, value in enumerate(conjugated(load_matrix(links[ph], (m,), x), t)):
                lower[ph, m, n, p, x + 1] = value

    def ahead_x(ph, n, x):
        return load_matrix(links[ph], (n,), 1) if x == 0 else load_matrix(x_in, (ph, n - 1))

    def pack_lanes(ph, m):
        for c in range(18):
            v0 = links[ph][m, c, 0]
            v1 = links[ph][m, c, 1]
            r0 = flip(v0)
            lane_out[ph, LANES.index(m), c] = jnp.where(low, v1, r0)
            lane_ahead[m, c, 0] = r0
            lane_ahead[m, c, 1] = flip(v1)

    def send_edges(ph, m):
        if m != 2:
            remote(ph, "z" + str(m)).start()
        if m in (1, 2):
            remote(ph, "x" + str(m)).start()

    def first_half(ph):
        field = links[ph]

        def shift_time(n, x):
            for c in range(18):
                v = field[n, c, x]
                time_ahead[n, c, x] = jnp.where(last_time, pltpu.roll(v, 63, 1), pltpu.roll(v, 127, 1))

        def mix(d, n, x, ahead):
            left = product(load_matrix(field, (n,), x), ahead)
            return dagger_product(load_matrix(field, (d,), x), left)

        def mix_z(n, x, ahead):
            store_matrix(mixed_z, (LANES.index(n),), (x + 1,), mix(2, n, x, ahead))

        def send_mixed(n):
            k = LANES.index(n)
            for c in range(18):
                mix_out[ph, k, c] = jnp.where(low, flip(mixed_z[k, c, 1]), mixed_z[k, c, 2])
            remote(ph, "mz" + str(n)).start()

        def seen_z(n, slot):
            k = LANES.index(n)
            remote(ph, "mz" + str(n)).wait_recv()
            for c in range(18):
                edge = mix_in[ph, k, c]
                mixed_z[k, c, 0] = jnp.where(low, edge, flip(mixed_z[k, c, 1]))
                mixed_z[k, c, 1] = jnp.where(low, flip(edge), flip(mixed_z[k, c, 2]))

            def seen(x):
                m, c = load_matrix(mixed_z, (k,), x), load_matrix(field, (n,), x)
                if ph == 1 and slot is not None:
                    traces[slot + x] = real_trace(m, c)
                for p, value in enumerate(twice_traceless(m, c) if n == 3 else twice_traceless(c, m)):
                    lower_z[k, p, x] = value
            loop(2, seen)

        def ahead_z(m):
            for c in range(18):
                edge = lane_in[ph, LANES.index(m), c]
                lane_ahead[m, c, 0] = jnp.where(low, lane_ahead[m, c, 0], edge)
                lane_ahead[m, c, 1] = jnp.where(low, lane_ahead[m, c, 1], flip(edge))

        loop(2, lambda x: shift_time(2, x))
        loop(2, lambda x: mix_z(3, x, load_matrix(time_ahead, (2,), x)))
        send_mixed(3)

        def pack_rows(x):
            for k, n in enumerate(ROWS):
                for c in range(18):
                    row_out[ph, k, c, x] = field[n, c, x, 0:1, :]
        loop(2, pack_rows)
        remote(ph, "y").start()
        if ph == 1:
            pl.semaphore_wait(known_sem.at[0], 2)
            known(1, -4, 4)

        loop(4, lambda i: shift_time(i // 2, lax.rem(i, 2)))

        def mix_x(x):
            store_matrix(mixed_x, (ph,), (x + 1,), mix(0, 3, x, load_matrix(time_ahead, (0,), x)))
        loop(2, mix_x)
        remote(ph, "mx").start()

        remote(ph, "y").wait_recv()

        def shift_rows(i):
            k, x = i // 2, lax.rem(i, 2)
            n = k + (k + 1) // 2
            for c in range(18):
                v = field[n, c, x]
                edge = jnp.broadcast_to(row_in[ph, k, c, x], (8, 128))
                row_ahead[n, c, x] = jnp.where(last_row, edge, pltpu.roll(v, 7, 0))
        loop(6, shift_rows)
        loop(2, lambda x: mix_z(1, x, load_matrix(row_ahead, (2,), x)))
        send_mixed(1)
        remote(ph, "x2").wait_recv()
        for x in range(2):
            mix_z(0, x, ahead_x(ph, 2, x))
        send_mixed(0)

        plane(ph, 1, 0, 0, load_matrix(row_ahead, (0,), 0), ahead_x(ph, 1, 0), 0)
        loop(2, lambda x: plane(
            ph, 1, 3, x, load_matrix(row_ahead, (3,), x), load_matrix(time_ahead, (1,), x), 2 + x))
        remote(ph, "x1").wait_recv()
        plane(ph, 1, 0, 1, load_matrix(row_ahead, (0,), 1), ahead_x(ph, 1, 1), 1)
        remote(ph, "lx1").start()

        remote(ph, "mx").wait_recv()

        def seen_x(x):
            m, c = load_matrix(mixed_x, (ph,), x), load_matrix(field, (3,), x)
            if ph == 1:
                traces[6 + x] = real_trace(m, c)
            for p, value in enumerate(twice_traceless(m, c)):
                lower[ph, 0, 3, p, x] = value
        loop(2, seen_x)
        remote(ph, "tx").start()

        seen_z(3, 8)
        remote(ph, "z0").wait_recv()
        if ph == 0:
            known(0, -2, 2)
        ahead_z(0)
        for x in (1, 0):
            plane(ph, 2, 0, x, load_matrix(lane_ahead, (0,), x), ahead_x(ph, 2, x), 10 + x)
            if x == 1:
                remote(ph, "lx2").start()
        remote(ph, "z1").wait_recv()
        ahead_z(1)
        loop(2, lambda x: plane(
            ph, 2, 1, x, load_matrix(lane_ahead, (1,), x), load_matrix(row_ahead, (2,), x), 4 + x, split=ph == 1))
        if ph == 1:
            total = traces[0]
            for slot in range(1, 12):
                total = total + traces[slot]
            gather_z[my_z] = jnp.sum(total, axis=0, keepdims=True)
            pl.semaphore_wait(known_sem.at[1], 2)
            for offset in range(1, half):
                z_sum(offset).start()
            known(2, half)
            loop(2, lambda x: below(ph, 2, 1, x, [loops[2, 1, p, x] for p in range(8)]))
        for k, m in enumerate(ROWS):
            for p in range(8):
                for x in range(2):
                    low_row_out[ph, k, p, x] = lower[ph, 1, m, p, x + 1, 7:8, :]
        remote(ph, "ly").start()

        def own_x(x):
            t = conjugated(dagger(load_matrix(field, (0,), x)), [lower[ph, 0, 3, p, x + 1] for p in range(8)])
            for p in range(8):
                loops[3, 0, p, x] = t[p]
            for p, value in enumerate(conjugated(load_matrix(field, (3,), x), t)):
                lower[ph, 3, 0, p, x + 1] = value
        remote(ph, "tx").wait_recv()
        loop(2, own_x)
        if ph == 1:
            for offset in range(1, half):
                z_sum(offset).wait_recv()
            total = gather_z[0]
            for source in range(1, half):
                total = total + gather_z[source]
            gather_rest[my_rest] = total
            pl.semaphore_wait(known_sem.at[2], 1)
            for offset in rest:
                rest_sum(offset).start()
        seen_z(1, None)
        seen_z(0, None)
        remote(ph, "z3").wait_recv()
        ahead_z(3)
        loop(2, lambda x: plane(
            ph, 3, 2, x, load_matrix(time_ahead, (2,), x), load_matrix(lane_ahead, (3,), x), None))

        for name in ("lx1", "lx2", "ly"):
            remote(ph, name).wait_recv()
    def half_step(ph, m, x):
        total = [None] * 8
        for n in range(4):
            if n == m:
                continue
            lead = LEAD[min(m, n), max(m, n)]
            first, second = (m, n) if lead == m else (n, m)
            for p in range(8):
                here = loops[first, second, p, x]
                if n == 0:
                    below_value = lower[ph, 0, m, p, x]
                elif n == 1:
                    edge = jnp.broadcast_to(low_row_in[ph, ROWS.index(m), p, x], (8, 128))
                    below_value = jnp.where(first_row, edge, pltpu.roll(lower[ph, 1, m, p, x + 1], 1, 0))
                elif n == 2:
                    below_value = lower_z[LANES.index(m), p, x]
                else:
                    value = lower[ph, 3, m, p, x + 1]
                    below_value = jnp.where(first_time, pltpu.roll(value, 65, 1), pltpu.roll(value, 1, 1))
                total[p] = add(total[p], here - below_value if lead == m else below_value - here)
        return [moment[m, PARTS[p], x] - (0.5 * KICK) * total[p] for p in range(8)]

    loads[2].wait()
    for m in (0, 1):
        loads[m].wait()
        pack_lanes(0, m)
    pl.semaphore_wait(barrier, len(neighbours))
    for m in (2, 0, 1):
        send_edges(0, m)
    loads[4].start()
    loads[3].wait()
    pack_lanes(0, 3)
    send_edges(0, 3)
    first_half(0)
    loads[4].wait()
    for m in (0, 2, 1, 3):
        def update(x):
            h = half_step(0, m, x)
            for p in range(8):
                moment[m, PARTS[p], x] = h[p]
            u = cayley(h, 0.5 * STEP)
            store_matrix(new_links, (m,), (x,), product(u, load_matrix(old_links, (m,), x)))
        loop(2, update)
        if m != 2:
            pack_lanes(1, m)
        send_edges(1, m)
    first_half(1)

    def finish(x):
        for m in range(4):
            h = half_step(1, m, x)
            for p in range(8):
                final[m, PARTS[p], x] = h[p]
            final[m, 17, x] = -(h[0] + h[1])
            for c, p in ((3, 2), (6, 4), (7, 6)):
                final[m, c, x] = -h[p]
                final[m, 9 + c, x] = h[p + 1]
            for c in (0, 4, 8):
                final[m, c, x] = jnp.zeros((8, 128), F32)
    loop(2, finish)

    for ph in range(2):
        for name in names:
            remote(ph, name).wait_send()
    for offset in range(1, half):
        z_sum(offset).wait_send()
    for offset in rest:
        rest_sum(offset).wait_send()
    for offset in rest:
        rest_sum(offset).wait_recv()
    total = gather_rest[0]
    for source in range(1, len(rest) + 1):
        total = total + gather_rest[source]
    volume = 72.0 * (2 * 8 * 128) * (sizes[0] * sizes[1] * sizes[2])
    plaquette[...] = jnp.broadcast_to(jnp.sum(total) * (4.0 / volume), (8, 128))


def solution(mesh):
    sizes = tuple(mesh.shape[name] for name in NAMES)
    spec = P(None, None, None, None, "gx", "gy", "zt")

    def step(gauge, momenta):
        shape = gauge.shape
        flat = (4, 18) + shape[4:]
        field = jax.ShapeDtypeStruct(flat, F32)
        dma = pltpu.SemaphoreType.DMA
        vmem = pl.BlockSpec(memory_space=pltpu.VMEM)
        half = sizes[2] // 2
        others = sizes[0] * sizes[1] * 2
        tile = (8, 128)

        def scratch(*lead):
            return pltpu.VMEM(lead + tile, F32)

        def rows(*lead):
            return pltpu.VMEM(lead + (1, 128), F32)

        links, final, plaquette = pl.pallas_call(
            lambda *refs: kernel(sizes, *refs),
            name="md_step",
            out_shape=(field, field, jax.ShapeDtypeStruct((8, 128), F32)),
            in_specs=[pl.BlockSpec(memory_space=pltpu.HBM)] * 2,
            out_specs=(vmem, vmem, vmem),
            scratch_shapes=[
                scratch(4, 18, 2), scratch(4, 18, 2), scratch(3, 18, 2), scratch(4, 18, 2), scratch(4, 18, 2),
                scratch(2, 18, 3), scratch(3, 18, 3),
                scratch(4, 4, 8, 2), scratch(2, 4, 4, 8, 3), scratch(3, 8, 2),
                rows(2, 3, 18, 2), rows(2, 3, 18, 2), scratch(2, 2, 18), scratch(2, 3, 18), scratch(2, 3, 18),
                scratch(2, 3, 18), scratch(2, 3, 18),
                rows(2, 3, 8, 2), rows(2, 3, 8, 2),
                scratch(12), rows(half), rows(others),
                dma((5,)), dma((2, 14)), dma((2, 14)), dma((half,)), dma((half,)), dma((others,)), dma((others,)),
                pltpu.SemaphoreType.REGULAR((3,)),
            ],
            compiler_params=pltpu.CompilerParams(collective_id=0, has_side_effects=True, vmem_limit_bytes=48 * 1024 * 1024),
        )(*(pltpu.with_memory_space_constraint(a.reshape(flat), pltpu.HBM) for a in (gauge, momenta)))
        return links.reshape(shape), final.reshape(shape), plaquette[0, 0]

    return jax.shard_map(step, mesh=mesh, in_specs=(spec, spec), out_specs=(spec, spec, P()), check_vma=False)
```

```python
import jax
import jax.numpy as jnp
from jax import lax
from jax.experimental import pallas as pl
from jax.experimental.pallas import tpu as pltpu
from jax.sharding import PartitionSpec as P

MESH = pl.DeviceIdType.MESH
F32 = jnp.float32
KICK = 0.25
STEP = 0.2
NAMES = ("gx", "gy", "zt")
LEAD = {(0, 1): 1, (0, 2): 2, (0, 3): 3, (1, 2): 2, (1, 3): 1, (2, 3): 3}


def load_matrix(ref, lead, *rest):
    return [[(ref[(*lead, 3 * i + j, *rest)], ref[(*lead, 9 + 3 * i + j, *rest)]) for j in range(3)] for i in range(3)]


def store_matrix(ref, lead, rest, value):
    for i in range(3):
        for j in range(3):
            for part in range(2):
                ref[(*lead, 9 * part + 3 * i + j, *rest)] = value[i][j][part]


def add(a, b):
    return b if a is None else a + b


def product(a, b):
    out = []
    for i in range(3):
        line = []
        for j in range(3):
            re, im = None, None
            for k in range(3):
                ar, ai = a[i][k]
                br, bi = b[k][j]
                re = add(re, ar * br - ai * bi)
                im = add(im, ar * bi + ai * br)
            line.append((re, im))
        out.append(line)
    return out


def dagger(a):
    return [[(a[j][i][0], -a[j][i][1]) for j in range(3)] for i in range(3)]


def dagger_product(a, b):
    out = []
    for i in range(3):
        line = []
        for j in range(3):
            re, im = None, None
            for k in range(3):
                ar, ai = a[k][i]
                br, bi = b[k][j]
                re = add(re, ar * br + ai * bi)
                im = add(im, ar * bi - ai * br)
            line.append((re, im))
        out.append(line)
    return out


def dagger_entry(x, y, i, j):
    re, im = None, None
    for k in range(3):
        ar, ai = x[i][k]
        br, bi = y[j][k]
        re = add(re, ar * br + ai * bi)
        im = add(im, ai * br - ar * bi)
    return re, im


def twice_traceless(x, y):
    diag = []
    for i in range(3):
        im = None
        for k in range(3):
            ar, ai = x[i][k]
            br, bi = y[i][k]
            im = add(im, ai * br - ar * bi)
        diag.append(im)
    mean = (diag[0] + diag[1] + diag[2]) * (2.0 / 3.0)
    out = [diag[0] + diag[0] - mean, diag[1] + diag[1] - mean]
    for i, j in ((0, 1), (0, 2), (1, 2)):
        pr, pi = dagger_entry(x, y, i, j)
        qr, qi = dagger_entry(x, y, j, i)
        out += [pr - qr, pi + qi]
    return out


def real_trace(x, y):
    total = None
    for i in range(3):
        for k in range(3):
            ar, ai = x[i][k]
            br, bi = y[i][k]
            total = add(total, ar * br + ai * bi)
    return total


def conjugated(d, t):
    d0, d1, ur, ui, vr, vi, wr, wi = t
    d2 = -(d0 + d1)

    def column(j):
        (ar, ai), (br, bi), (cr, ci) = d[0][j], d[1][j], d[2][j]
        first = (
            ur * br - ui * bi + (vr * cr - vi * ci) - d0 * ai,
            ur * bi + ui * br + (vr * ci + vi * cr) + d0 * ar,
        )
        second = (
            wr * cr - wi * ci - (ur * ar + ui * ai) - d1 * bi,
            wr * ci + wi * cr + (ui * ar - ur * ai) + d1 * br,
        )
        third = (
            -(vr * ar + vi * ai) - (wr * br + wi * bi) - d2 * ci,
            (vi * ar - vr * ai) + (wi * br - wr * bi) + d2 * cr,
        )
        return first, second, third

    def imag(i, col):
        total = None
        for k in range(3):
            ar, ai = d[k][i]
            total = add(total, ar * col[k][1] - ai * col[k][0])
        return total

    def entry(i, col):
        re, im = None, None
        for k in range(3):
            ar, ai = d[k][i]
            br, bi = col[k]
            re = add(re, ar * br + ai * bi)
            im = add(im, ar * bi - ai * br)
        return re, im

    zero = column(0)
    e0 = imag(0, zero)
    one = column(1)
    e1 = imag(1, one)
    u = entry(0, one)
    two = column(2)
    v = entry(0, two)
    w = entry(1, two)
    return [e0, e1, u[0], u[1], v[0], v[1], w[0], w[1]]


def cayley(h, scale):
    a0, a1, ur, ui, vr, vi, wr, wi = [scale * part for part in h]
    a2 = -(a0 + a1)
    uu = ur * ur + ui * ui
    vv = vr * vr + vi * vi
    ww = wr * wr + wi * wi
    s00, s11, s22 = a0 * a0, a1 * a1, a2 * a2
    one_s = 1.0 + (0.5 * (s00 + s11 + s22) + (uu + vv + ww))
    uwr, uwi = ur * wr - ui * wi, ur * wi + ui * wr
    det_h = a0 * a1 * a2 + 2.0 * (uwi * vr - uwr * vi) - a0 * ww - a1 * vv - a2 * uu
    scale2 = 2.0 / (one_s * one_s + det_h * det_h)
    qr, qi = one_s * scale2, -(det_h * scale2)
    pr, pi = a2 * ui - (vr * wr + vi * wi), -(a2 * ur) - (vi * wr - vr * wi)
    rr, ri = a1 * vi + uwr, uwi - a1 * vr
    tr, ti = a0 * wi - (ur * vr + ui * vi), -(a0 * wr) - (ur * vi - ui * vr)
    rows = [
        [(one_s - (s00 + uu + vv), a0), (ur + pr, ui + pi), (vr + rr, vi + ri)],
        [(pr - ur, ui - pi), (one_s - (s11 + uu + ww), a1), (wr + tr, wi + ti)],
        [(rr - vr, vi - ri), (tr - wr, wi - ti), (one_s - (s22 + vv + ww), a2)],
    ]
    out = []
    for i in range(3):
        line = []
        for j in range(3):
            br, bi = rows[i][j]
            re, im = br * qr - bi * qi, br * qi + bi * qr
            line.append((re - 1.0 if i == j else re, im))
        out.append(line)
    return out


PARTS = (9, 13, 1, 10, 2, 11, 5, 14)
ROWS = (0, 2, 3)
LANES = (0, 1, 3)


def kernel(
    sizes, gauge, momenta, new_links, final, plaquette,
    old_links, moment, time_ahead, row_ahead, lane_ahead, mixed_x, mixed_z,
    loops, lower, lower_z,
    row_out, row_in, x_in, lane_out, lane_in, mix_out, mix_in,
    low_row_out, low_row_in,
    traces, gather_z, gather_rest,
    load_sem, send_sem, recv_sem, z_send, z_recv, rest_send, rest_recv, known_sem,
):
    me = [lax.axis_index(name) for name in NAMES]
    links = (old_links, new_links)
    half = sizes[2] // 2
    my_half, my_z = me[2] // half, lax.rem(me[2], half)

    def peer(axis, offset):
        return {NAMES[axis]: lax.rem(me[axis] + (offset + sizes[axis]), sizes[axis])}

    def z_peer(offset):
        return {"zt": my_half * half + lax.rem(my_z + offset, half)}

    rest = [(i, j, k) for i in range(sizes[0]) for j in range(sizes[1]) for k in range(2) if i + j + k]

    def rest_peer(offset):
        i, j, k = offset
        return {**peer(0, i), **peer(1, j), "zt": lax.rem(my_half + k, 2) * half + my_z}

    barrier = pltpu.get_barrier_semaphore()
    neighbours = [peer(axis, offset) for axis in range(3) for offset in (-1, 1)]
    for device in neighbours:
        pl.semaphore_signal(barrier, inc=1, device_id=device, device_id_type=MESH)

    loads = {m: pltpu.make_async_copy(gauge.at[m], old_links.at[m], load_sem.at[m]) for m in (2, 0, 1, 3)}
    for copy in loads.values():
        copy.start()
    loads[4] = pltpu.make_async_copy(momenta, moment, load_sem.at[4])

    def known(step, *offsets):
        for offset in offsets:
            pl.semaphore_signal(known_sem.at[step], inc=1, device_id=peer(2, offset), device_id_type=MESH)

    lane = lax.broadcasted_iota(jnp.int32, (8, 128), 1)
    row = lax.broadcasted_iota(jnp.int32, (8, 128), 0)
    low = lane < 64
    time = lax.rem(lane, 64)
    last_time = time == 63
    first_time = time == 0
    last_row = row == 7
    first_row = row == 0

    def flip(value):
        return pltpu.roll(value, 64, 1)

    def remote(ph, name):
        now = links[ph]
        number, src, dst, axis, offset = {
            "x1": (0, now.at[1, :, 0], x_in.at[ph, 0], 0, -1),
            "x2": (1, now.at[2, :, 0], x_in.at[ph, 1], 0, -1),
            "y": (2, row_out.at[ph], row_in.at[ph], 1, -1),
            "z0": (3, lane_out.at[ph, 0], lane_in.at[ph, 0], 2, -1),
            "z1": (4, lane_out.at[ph, 1], lane_in.at[ph, 1], 2, -1),
            "z3": (5, lane_out.at[ph, 2], lane_in.at[ph, 2], 2, -1),
            "mx": (6, mixed_x.at[ph, :, 2], mixed_x.at[ph, :, 0], 0, 1),
            "mz0": (7, mix_out.at[ph, 0], mix_in.at[ph, 0], 2, 1),
            "mz1": (8, mix_out.at[ph, 1], mix_in.at[ph, 1], 2, 1),
            "mz3": (9, mix_out.at[ph, 2], mix_in.at[ph, 2], 2, 1),
            "lx1": (10, lower.at[ph, 0, 1, :, 2], lower.at[ph, 0, 1, :, 0], 0, 1),
            "lx2": (11, lower.at[ph, 0, 2, :, 2], lower.at[ph, 0, 2, :, 0], 0, 1),
            "ly": (12, low_row_out.at[ph], low_row_in.at[ph], 1, 1),
            "tx": (13, lower.at[ph, 0, 3, :, 0], lower.at[ph, 0, 3, :, 2], 0, -1),
        }[name]
        return pltpu.make_async_remote_copy(
            src_ref=src, dst_ref=dst, send_sem=send_sem.at[ph, number], recv_sem=recv_sem.at[ph, number],
            device_id=peer(axis, offset), device_id_type=MESH)

    names = ("x1", "x2", "y", "z0", "z1", "z3", "mx", "mz0", "mz1", "mz3", "lx1", "lx2", "ly", "tx")

    def z_sum(offset):
        return pltpu.make_async_remote_copy(
            src_ref=gather_z.at[my_z], dst_ref=gather_z.at[my_z],
            send_sem=z_send.at[offset], recv_sem=z_recv.at[offset],
            device_id=z_peer(offset), device_id_type=MESH)

    my_rest = (me[0] * sizes[1] + me[1]) * 2 + my_half

    def rest_sum(offset):
        number = (offset[0] * sizes[1] + offset[1]) * 2 + offset[2]
        return pltpu.make_async_remote_copy(
            src_ref=gather_rest.at[my_rest], dst_ref=gather_rest.at[my_rest],
            send_sem=rest_send.at[number], recv_sem=rest_recv.at[number],
            device_id=rest_peer(offset), device_id_type=MESH)

    def loop(count, body):
        def step(i, _):
            body(i)
            return 0
        lax.fori_loop(0, count, step, 0)

    def plane(ph, m, n, x, b, c, slot, split=False):
        a = load_matrix(links[ph], (m,), x)
        left = product(a, b)
        d = load_matrix(links[ph], (n,), x)
        right = product(d, c)
        t = twice_traceless(left, right)
        if ph == 1 and slot is not None:
            traces[slot] = real_trace(left, right)
        for p in range(8):
            loops[m, n, p, x] = t[p]
        if not split:
            below(ph, m, n, x, t)

    def below(ph, m, n, x, t):
        if n != 2:
            for p, value in enumerate(conjugated(load_matrix(links[ph], (n,), x), t)):
                lower[ph, n, m, p, x + 1] = value
        if m != 2:
            for p, value in enumerate(conjugated(load_matrix(links[ph], (m,), x), t)):
                lower[ph, m, n, p, x + 1] = value

    def ahead_x(ph, n, x):
        return load_matrix(links[ph], (n,), 1) if x == 0 else load_matrix(x_in, (ph, n - 1))

    def pack_lanes(ph, m):
        for c in range(18):
            v0 = links[ph][m, c, 0]
            v1 = links[ph][m, c, 1]
            r0 = flip(v0)
            lane_out[ph, LANES.index(m), c] = jnp.where(low, v1, r0)
            lane_ahead[m, c, 0] = r0
            lane_ahead[m, c, 1] = flip(v1)

    def send_rows(ph):
        def pack_rows(x):
            for k, n in enumerate(ROWS):
                for c in range(18):
                    row_out[ph, k, c, x] = links[ph][n, c, x, 0:1, :]
        loop(2, pack_rows)

    def first_half(ph):
        field = links[ph]

        def shift_time(n, x):
            for c in range(18):
                v = field[n, c, x]
                time_ahead[n, c, x] = jnp.where(last_time, pltpu.roll(v, 63, 1), pltpu.roll(v, 127, 1))

        def mix(d, n, x, ahead):
            left = product(load_matrix(field, (n,), x), ahead)
            return dagger_product(load_matrix(field, (d,), x), left)

        def mix_z(n, x, ahead):
            store_matrix(mixed_z, (LANES.index(n),), (x + 1,), mix(2, n, x, ahead))

        def send_mixed(n):
            k = LANES.index(n)
            for c in range(18):
                mix_out[ph, k, c] = jnp.where(low, flip(mixed_z[k, c, 1]), mixed_z[k, c, 2])
            remote(ph, "mz" + str(n)).start()

        def seen_z(n, slot):
            k = LANES.index(n)
            remote(ph, "mz" + str(n)).wait_recv()
            for c in range(18):
                edge = mix_in[ph, k, c]
                mixed_z[k, c, 0] = jnp.where(low, edge, flip(mixed_z[k, c, 1]))
                mixed_z[k, c, 1] = jnp.where(low, flip(edge), flip(mixed_z[k, c, 2]))

            def seen(x):
                m, c = load_matrix(mixed_z, (k,), x), load_matrix(field, (n,), x)
                if ph == 1 and slot is not None:
                    traces[slot + x] = real_trace(m, c)
                for p, value in enumerate(twice_traceless(m, c) if n == 3 else twice_traceless(c, m)):
                    lower_z[k, p, x] = value
            loop(2, seen)

        def ahead_z(m):
            for c in range(18):
                edge = lane_in[ph, LANES.index(m), c]
                lane_ahead[m, c, 0] = jnp.where(low, lane_ahead[m, c, 0], edge)
                lane_ahead[m, c, 1] = jnp.where(low, lane_ahead[m, c, 1], flip(edge))

        loop(2, lambda x: shift_time(2, x))
        loop(2, lambda x: mix_z(3, x, load_matrix(time_ahead, (2,), x)))
        send_mixed(3)
        pack_lanes(ph, 3)
        remote(ph, "z3").start()
        if ph == 1:
            pl.semaphore_wait(known_sem.at[0], 2)
            known(1, -4, 4)

        loop(4, lambda i: shift_time(i // 2, lax.rem(i, 2)))

        def mix_x(x):
            store_matrix(mixed_x, (ph,), (x + 1,), mix(0, 3, x, load_matrix(time_ahead, (0,), x)))
        loop(2, mix_x)
        remote(ph, "mx").start()

        remote(ph, "y").wait_recv()

        def shift_rows(i):
            k, x = i // 2, lax.rem(i, 2)
            n = k + (k + 1) // 2
            for c in range(18):
                v = field[n, c, x]
                edge = jnp.broadcast_to(row_in[ph, k, c, x], (8, 128))
                row_ahead[n, c, x] = jnp.where(last_row, edge, pltpu.roll(v, 7, 0))
        loop(6, shift_rows)
        loop(2, lambda x: mix_z(1, x, load_matrix(row_ahead, (2,), x)))
        send_mixed(1)
        remote(ph, "x2").wait_recv()
        for x in range(2):
            mix_z(0, x, ahead_x(ph, 2, x))
        send_mixed(0)

        plane(ph, 1, 0, 0, load_matrix(row_ahead, (0,), 0), ahead_x(ph, 1, 0), 0)
        loop(2, lambda x: plane(
            ph, 1, 3, x, load_matrix(row_ahead, (3,), x), load_matrix(time_ahead, (1,), x), 2 + x))
        remote(ph, "x1").wait_recv()
        plane(ph, 1, 0, 1, load_matrix(row_ahead, (0,), 1), ahead_x(ph, 1, 1), 1)
        remote(ph, "lx1").start()

        remote(ph, "mx").wait_recv()

        def seen_x(x):
            m, c = load_matrix(mixed_x, (ph,), x), load_matrix(field, (3,), x)
            if ph == 1:
                traces[6 + x] = real_trace(m, c)
            for p, value in enumerate(twice_traceless(m, c)):
                lower[ph, 0, 3, p, x] = value
        loop(2, seen_x)
        remote(ph, "tx").start()

        seen_z(3, 8)
        remote(ph, "z0").wait_recv()
        if ph == 0:
            known(0, -2, 2)
        ahead_z(0)
        for x in (1, 0):
            plane(ph, 2, 0, x, load_matrix(lane_ahead, (0,), x), ahead_x(ph, 2, x), 10 + x)
            if x == 1:
                remote(ph, "lx2").start()
        remote(ph, "z1").wait_recv()
        ahead_z(1)
        loop(2, lambda x: plane(
            ph, 2, 1, x, load_matrix(lane_ahead, (1,), x), load_matrix(row_ahead, (2,), x), 4 + x, split=ph == 1))
        if ph == 1:
            total = traces[0]
            for slot in range(1, 12):
                total = total + traces[slot]
            gather_z[my_z] = jnp.sum(total, axis=0, keepdims=True)
            pl.semaphore_wait(known_sem.at[1], 2)
            for offset in range(1, half):
                z_sum(offset).start()
            known(2, half)
            loop(2, lambda x: below(ph, 2, 1, x, [loops[2, 1, p, x] for p in range(8)]))
        for k, m in enumerate(ROWS):
            for p in range(8):
                for x in range(2):
                    low_row_out[ph, k, p, x] = lower[ph, 1, m, p, x + 1, 7:8, :]
        remote(ph, "ly").start()

        def own_x(x):
            t = conjugated(dagger(load_matrix(field, (0,), x)), [lower[ph, 0, 3, p, x + 1] for p in range(8)])
            for p in range(8):
                loops[3, 0, p, x] = t[p]
            for p, value in enumerate(conjugated(load_matrix(field, (3,), x), t)):
                lower[ph, 3, 0, p, x + 1] = value
        remote(ph, "tx").wait_recv()
        loop(2, own_x)
        if ph == 1:
            for offset in range(1, half):
                z_sum(offset).wait_recv()
            total = gather_z[0]
            for source in range(1, half):
                total = total + gather_z[source]
            gather_rest[my_rest] = total
            pl.semaphore_wait(known_sem.at[2], 1)
            for offset in rest:
                rest_sum(offset).start()
        seen_z(1, None)
        seen_z(0, None)
        remote(ph, "z3").wait_recv()
        ahead_z(3)
        loop(2, lambda x: plane(
            ph, 3, 2, x, load_matrix(time_ahead, (2,), x), load_matrix(lane_ahead, (3,), x), None))

        for name in ("lx1", "lx2", "ly"):
            remote(ph, name).wait_recv()
    def half_step(ph, m, x):
        total = [None] * 8
        for n in range(4):
            if n == m:
                continue
            lead = LEAD[min(m, n), max(m, n)]
            first, second = (m, n) if lead == m else (n, m)
            for p in range(8):
                here = loops[first, second, p, x]
                if n == 0:
                    below_value = lower[ph, 0, m, p, x]
                elif n == 1:
                    edge = jnp.broadcast_to(low_row_in[ph, ROWS.index(m), p, x], (8, 128))
                    below_value = jnp.where(first_row, edge, pltpu.roll(lower[ph, 1, m, p, x + 1], 1, 0))
                elif n == 2:
                    below_value = lower_z[LANES.index(m), p, x]
                else:
                    value = lower[ph, 3, m, p, x + 1]
                    below_value = jnp.where(first_time, pltpu.roll(value, 65, 1), pltpu.roll(value, 1, 1))
                total[p] = add(total[p], here - below_value if lead == m else below_value - here)
        return [moment[m, PARTS[p], x] - (0.5 * KICK) * total[p] for p in range(8)]

    for m in range(4):
        loads[m].wait()
    send_rows(0)
    pack_lanes(0, 0)
    pl.semaphore_wait(barrier, len(neighbours))
    for name in ("y", "x2", "z0"):
        remote(0, name).start()
    pack_lanes(0, 1)
    for name in ("z1", "x1"):
        remote(0, name).start()
    loads[4].start()
    first_half(0)
    loads[4].wait()
    for m in (2, 0, 3, 1):
        def update(x):
            h = half_step(0, m, x)
            for p in range(8):
                moment[m, PARTS[p], x] = h[p]
            u = cayley(h, 0.5 * STEP)
            store_matrix(new_links, (m,), (x,), product(u, load_matrix(old_links, (m,), x)))
        loop(2, update)
        if m == 2:
            remote(1, "x2").start()
        elif m == 3:
            send_rows(1)
            pack_lanes(1, 0)
            remote(1, "y").start()
            remote(1, "z0").start()
        elif m == 1:
            pack_lanes(1, 1)
            remote(1, "z1").start()
            remote(1, "x1").start()
    first_half(1)

    def finish(x):
        for m in range(4):
            h = half_step(1, m, x)
            for p in range(8):
                final[m, PARTS[p], x] = h[p]
            final[m, 17, x] = -(h[0] + h[1])
            for c, p in ((3, 2), (6, 4), (7, 6)):
                final[m, c, x] = -h[p]
                final[m, 9 + c, x] = h[p + 1]
            for c in (0, 4, 8):
                final[m, c, x] = jnp.zeros((8, 128), F32)
    loop(2, finish)

    for ph in range(2):
        for name in names:
            remote(ph, name).wait_send()
    for offset in range(1, half):
        z_sum(offset).wait_send()
    for offset in rest:
        rest_sum(offset).wait_send()
    for offset in rest:
        rest_sum(offset).wait_recv()
    total = gather_rest[0]
    for source in range(1, len(rest) + 1):
        total = total + gather_rest[source]
    volume = 72.0 * (2 * 8 * 128) * (sizes[0] * sizes[1] * sizes[2])
    plaquette[...] = jnp.broadcast_to(jnp.sum(total) * (4.0 / volume), (8, 128))


def solution(mesh):
    sizes = tuple(mesh.shape[name] for name in NAMES)
    spec = P(None, None, None, None, "gx", "gy", "zt")

    def step(gauge, momenta):
        shape = gauge.shape
        flat = (4, 18) + shape[4:]
        field = jax.ShapeDtypeStruct(flat, F32)
        dma = pltpu.SemaphoreType.DMA
        vmem = pl.BlockSpec(memory_space=pltpu.VMEM)
        half = sizes[2] // 2
        others = sizes[0] * sizes[1] * 2
        tile = (8, 128)

        def scratch(*lead):
            return pltpu.VMEM(lead + tile, F32)

        def rows(*lead):
            return pltpu.VMEM(lead + (1, 128), F32)

        links, final, plaquette = pl.pallas_call(
            lambda *refs: kernel(sizes, *refs),
            name="md_step",
            out_shape=(field, field, jax.ShapeDtypeStruct((8, 128), F32)),
            in_specs=[pl.BlockSpec(memory_space=pltpu.HBM)] * 2,
            out_specs=(vmem, vmem, vmem),
            scratch_shapes=[
                scratch(4, 18, 2), scratch(4, 18, 2), scratch(3, 18, 2), scratch(4, 18, 2), scratch(4, 18, 2),
                scratch(2, 18, 3), scratch(3, 18, 3),
                scratch(4, 4, 8, 2), scratch(2, 4, 4, 8, 3), scratch(3, 8, 2),
                rows(2, 3, 18, 2), rows(2, 3, 18, 2), scratch(2, 2, 18), scratch(2, 3, 18), scratch(2, 3, 18),
                scratch(2, 3, 18), scratch(2, 3, 18),
                rows(2, 3, 8, 2), rows(2, 3, 8, 2),
                scratch(12), rows(half), rows(others),
                dma((5,)), dma((2, 14)), dma((2, 14)), dma((half,)), dma((half,)), dma((others,)), dma((others,)),
                pltpu.SemaphoreType.REGULAR((3,)),
            ],
            compiler_params=pltpu.CompilerParams(collective_id=0, has_side_effects=True, vmem_limit_bytes=48 * 1024 * 1024),
        )(*(pltpu.with_memory_space_constraint(a.reshape(flat), pltpu.HBM) for a in (gauge, momenta)))
        return links.reshape(shape), final.reshape(shape), plaquette[0, 0]

    return jax.shard_map(step, mesh=mesh, in_specs=(spec, spec), out_specs=(spec, spec, P()), check_vma=False)
```

```python
import jax
import jax.numpy as jnp
from jax import lax
from jax.experimental import pallas as pl
from jax.experimental.pallas import tpu as pltpu
from jax.sharding import PartitionSpec as P

MESH = pl.DeviceIdType.MESH
F32 = jnp.float32
KICK = 0.25
STEP = 0.2
NAMES = ("gx", "gy", "zt")
LEAD = {(0, 1): 1, (0, 2): 2, (0, 3): 3, (1, 2): 2, (1, 3): 1, (2, 3): 3}


def load_matrix(ref, lead, *rest):
    return [[(ref[(*lead, 3 * i + j, *rest)], ref[(*lead, 9 + 3 * i + j, *rest)]) for j in range(3)] for i in range(3)]


def store_matrix(ref, lead, rest, value):
    for i in range(3):
        for j in range(3):
            for part in range(2):
                ref[(*lead, 9 * part + 3 * i + j, *rest)] = value[i][j][part]


def add(a, b):
    return b if a is None else a + b


def product(a, b):
    out = []
    for i in range(3):
        line = []
        for j in range(3):
            re, im = None, None
            for k in range(3):
                ar, ai = a[i][k]
                br, bi = b[k][j]
                re = add(re, ar * br - ai * bi)
                im = add(im, ar * bi + ai * br)
            line.append((re, im))
        out.append(line)
    return out


def dagger(a):
    return [[(a[j][i][0], -a[j][i][1]) for j in range(3)] for i in range(3)]


def dagger_product(a, b):
    out = []
    for i in range(3):
        line = []
        for j in range(3):
            re, im = None, None
            for k in range(3):
                ar, ai = a[k][i]
                br, bi = b[k][j]
                re = add(re, ar * br + ai * bi)
                im = add(im, ar * bi - ai * br)
            line.append((re, im))
        out.append(line)
    return out


def dagger_entry(x, y, i, j):
    re, im = None, None
    for k in range(3):
        ar, ai = x[i][k]
        br, bi = y[j][k]
        re = add(re, ar * br + ai * bi)
        im = add(im, ai * br - ar * bi)
    return re, im


def twice_traceless(x, y):
    diag = []
    for i in range(3):
        im = None
        for k in range(3):
            ar, ai = x[i][k]
            br, bi = y[i][k]
            im = add(im, ai * br - ar * bi)
        diag.append(im)
    mean = (diag[0] + diag[1] + diag[2]) * (2.0 / 3.0)
    out = [diag[0] + diag[0] - mean, diag[1] + diag[1] - mean]
    for i, j in ((0, 1), (0, 2), (1, 2)):
        pr, pi = dagger_entry(x, y, i, j)
        qr, qi = dagger_entry(x, y, j, i)
        out += [pr - qr, pi + qi]
    return out


def real_trace(x, y):
    total = None
    for i in range(3):
        for k in range(3):
            ar, ai = x[i][k]
            br, bi = y[i][k]
            total = add(total, ar * br + ai * bi)
    return total


def conjugated(d, t):
    d0, d1, ur, ui, vr, vi, wr, wi = t
    d2 = -(d0 + d1)

    def column(j):
        (ar, ai), (br, bi), (cr, ci) = d[0][j], d[1][j], d[2][j]
        first = (
            ur * br - ui * bi + (vr * cr - vi * ci) - d0 * ai,
            ur * bi + ui * br + (vr * ci + vi * cr) + d0 * ar,
        )
        second = (
            wr * cr - wi * ci - (ur * ar + ui * ai) - d1 * bi,
            wr * ci + wi * cr + (ui * ar - ur * ai) + d1 * br,
        )
        third = (
            -(vr * ar + vi * ai) - (wr * br + wi * bi) - d2 * ci,
            (vi * ar - vr * ai) + (wi * br - wr * bi) + d2 * cr,
        )
        return first, second, third

    def imag(i, col):
        total = None
        for k in range(3):
            ar, ai = d[k][i]
            total = add(total, ar * col[k][1] - ai * col[k][0])
        return total

    def entry(i, col):
        re, im = None, None
        for k in range(3):
            ar, ai = d[k][i]
            br, bi = col[k]
            re = add(re, ar * br + ai * bi)
            im = add(im, ar * bi - ai * br)
        return re, im

    zero = column(0)
    e0 = imag(0, zero)
    one = column(1)
    e1 = imag(1, one)
    u = entry(0, one)
    two = column(2)
    v = entry(0, two)
    w = entry(1, two)
    return [e0, e1, u[0], u[1], v[0], v[1], w[0], w[1]]


def cayley(h, scale):
    a0, a1, ur, ui, vr, vi, wr, wi = [scale * part for part in h]
    a2 = -(a0 + a1)
    uu = ur * ur + ui * ui
    vv = vr * vr + vi * vi
    ww = wr * wr + wi * wi
    s00, s11, s22 = a0 * a0, a1 * a1, a2 * a2
    one_s = 1.0 + (0.5 * (s00 + s11 + s22) + (uu + vv + ww))
    uwr, uwi = ur * wr - ui * wi, ur * wi + ui * wr
    det_h = a0 * a1 * a2 + 2.0 * (uwi * vr - uwr * vi) - a0 * ww - a1 * vv - a2 * uu
    scale2 = 2.0 / (one_s * one_s + det_h * det_h)
    qr, qi = one_s * scale2, -(det_h * scale2)
    pr, pi = a2 * ui - (vr * wr + vi * wi), -(a2 * ur) - (vi * wr - vr * wi)
    rr, ri = a1 * vi + uwr, uwi - a1 * vr
    tr, ti = a0 * wi - (ur * vr + ui * vi), -(a0 * wr) - (ur * vi - ui * vr)
    rows = [
        [(one_s - (s00 + uu + vv), a0), (ur + pr, ui + pi), (vr + rr, vi + ri)],
        [(pr - ur, ui - pi), (one_s - (s11 + uu + ww), a1), (wr + tr, wi + ti)],
        [(rr - vr, vi - ri), (tr - wr, wi - ti), (one_s - (s22 + vv + ww), a2)],
    ]
    out = []
    for i in range(3):
        line = []
        for j in range(3):
            br, bi = rows[i][j]
            re, im = br * qr - bi * qi, br * qi + bi * qr
            line.append((re - 1.0 if i == j else re, im))
        out.append(line)
    return out


PARTS = (9, 13, 1, 10, 2, 11, 5, 14)
ROWS = (0, 2, 3)
LANES = (0, 1, 3)


def kernel(
    sizes, gauge, momenta, fields, plaquette,
    old_links, moment, time_ahead, row_ahead, lane_ahead, mixed_x, mixed_z,
    loops, lower, lower_z,
    row_out, row_in, x_in, lane_out, lane_in, mix_out, mix_in,
    low_row_out, low_row_in,
    traces, gather_z, gather_rest,
    load_sem, send_sem, recv_sem, z_send, z_recv, rest_send, rest_recv, known_sem,
):
    me = [lax.axis_index(name) for name in NAMES]
    new_links, final = fields.at[0], fields.at[1]
    links = (old_links, new_links)
    half = sizes[2] // 2
    my_half, my_z = me[2] // half, lax.rem(me[2], half)

    def peer(axis, offset):
        return {NAMES[axis]: lax.rem(me[axis] + (offset + sizes[axis]), sizes[axis])}

    def z_peer(offset):
        return {"zt": my_half * half + lax.rem(my_z + offset, half)}

    rest = [(i, j, k) for i in range(sizes[0]) for j in range(sizes[1]) for k in range(2) if i + j + k]

    def rest_peer(offset):
        i, j, k = offset
        return {**peer(0, i), **peer(1, j), "zt": lax.rem(my_half + k, 2) * half + my_z}

    barrier = pltpu.get_barrier_semaphore()
    neighbours = [peer(axis, offset) for axis in range(3) for offset in (-1, 1)]
    for device in neighbours:
        pl.semaphore_signal(barrier, inc=1, device_id=device, device_id_type=MESH)

    loads = {m: pltpu.make_async_copy(gauge.at[m], old_links.at[m], load_sem.at[m]) for m in (2, 0, 1, 3)}
    for copy in loads.values():
        copy.start()
    loads[4] = pltpu.make_async_copy(momenta, moment, load_sem.at[4])

    def known(step, *offsets):
        for offset in offsets:
            pl.semaphore_signal(known_sem.at[step], inc=1, device_id=peer(2, offset), device_id_type=MESH)

    lane = lax.broadcasted_iota(jnp.int32, (8, 128), 1)
    row = lax.broadcasted_iota(jnp.int32, (8, 128), 0)
    low = lane < 64
    time = lax.rem(lane, 64)
    last_time = time == 63
    first_time = time == 0
    last_row = row == 7
    first_row = row == 0

    def flip(value):
        return pltpu.roll(value, 64, 1)

    def remote(ph, name):
        now = links[ph]
        number, src, dst, axis, offset = {
            "x1": (0, now.at[1, :, 0], x_in.at[ph, 0], 0, -1),
            "x2": (1, now.at[2, :, 0], x_in.at[ph, 1], 0, -1),
            "y": (2, row_out.at[ph], row_in.at[ph], 1, -1),
            "z0": (3, lane_out.at[ph, 0], lane_in.at[ph, 0], 2, -1),
            "z1": (4, lane_out.at[ph, 1], lane_in.at[ph, 1], 2, -1),
            "z3": (5, lane_out.at[ph, 2], lane_in.at[ph, 2], 2, -1),
            "mx": (6, mixed_x.at[ph, :, 2], mixed_x.at[ph, :, 0], 0, 1),
            "mz0": (7, mix_out.at[ph, 0], mix_in.at[ph, 0], 2, 1),
            "mz1": (8, mix_out.at[ph, 1], mix_in.at[ph, 1], 2, 1),
            "mz3": (9, mix_out.at[ph, 2], mix_in.at[ph, 2], 2, 1),
            "lx1": (10, lower.at[ph, 0, 1, :, 2], lower.at[ph, 0, 1, :, 0], 0, 1),
            "lx2": (11, lower.at[ph, 0, 2, :, 2], lower.at[ph, 0, 2, :, 0], 0, 1),
            "ly": (12, low_row_out.at[ph], low_row_in.at[ph], 1, 1),
            "tx": (13, lower.at[ph, 0, 3, :, 0], lower.at[ph, 0, 3, :, 2], 0, -1),
        }[name]
        return pltpu.make_async_remote_copy(
            src_ref=src, dst_ref=dst, send_sem=send_sem.at[ph, number], recv_sem=recv_sem.at[ph, number],
            device_id=peer(axis, offset), device_id_type=MESH)

    names = ("x1", "x2", "y", "z0", "z1", "z3", "mx", "mz0", "mz1", "mz3", "lx1", "lx2", "ly", "tx")

    def z_sum(offset):
        return pltpu.make_async_remote_copy(
            src_ref=gather_z.at[my_z], dst_ref=gather_z.at[my_z],
            send_sem=z_send.at[offset], recv_sem=z_recv.at[offset],
            device_id=z_peer(offset), device_id_type=MESH)

    my_rest = (me[0] * sizes[1] + me[1]) * 2 + my_half

    def rest_sum(offset):
        number = (offset[0] * sizes[1] + offset[1]) * 2 + offset[2]
        return pltpu.make_async_remote_copy(
            src_ref=gather_rest.at[my_rest], dst_ref=gather_rest.at[my_rest],
            send_sem=rest_send.at[number], recv_sem=rest_recv.at[number],
            device_id=rest_peer(offset), device_id_type=MESH)

    def loop(count, body):
        def step(i, _):
            body(i)
            return 0
        lax.fori_loop(0, count, step, 0)

    def plane(ph, m, n, x, b, c, slot, split=False):
        a = load_matrix(links[ph], (m,), x)
        left = product(a, b)
        d = load_matrix(links[ph], (n,), x)
        right = product(d, c)
        t = twice_traceless(left, right)
        if ph == 1 and slot is not None:
            traces[slot] = real_trace(left, right)
        for p in range(8):
            loops[m, n, p, x] = t[p]
        if not split:
            below(ph, m, n, x, t)

    def below(ph, m, n, x, t):
        if n != 2:
            for p, value in enumerate(conjugated(load_matrix(links[ph], (n,), x), t)):
                lower[ph, n, m, p, x + 1] = value
        if m != 2:
            for p, value in enumerate(conjugated(load_matrix(links[ph], (m,), x), t)):
                lower[ph, m, n, p, x + 1] = value

    def ahead_x(ph, n, x):
        return load_matrix(links[ph], (n,), 1) if x == 0 else load_matrix(x_in, (ph, n - 1))

    def pack_lanes(ph, m):
        for c in range(18):
            v0 = links[ph][m, c, 0]
            v1 = links[ph][m, c, 1]
            r0 = flip(v0)
            lane_out[ph, LANES.index(m), c] = jnp.where(low, v1, r0)
            lane_ahead[m, c, 0] = r0
            lane_ahead[m, c, 1] = flip(v1)

    def send_rows(ph):
        def pack_rows(x):
            for k, n in enumerate(ROWS):
                for c in range(18):
                    row_out[ph, k, c, x] = links[ph][n, c, x, 0:1, :]
        loop(2, pack_rows)

    def first_half(ph):
        field = links[ph]

        def shift_time(n, x):
            for c in range(18):
                v = field[n, c, x]
                time_ahead[n, c, x] = jnp.where(last_time, pltpu.roll(v, 63, 1), pltpu.roll(v, 127, 1))

        def mix(d, n, x, ahead):
            left = product(load_matrix(field, (n,), x), ahead)
            return dagger_product(load_matrix(field, (d,), x), left)

        def mix_z(n, x, ahead):
            store_matrix(mixed_z, (LANES.index(n),), (x + 1,), mix(2, n, x, ahead))

        def send_mixed(n):
            k = LANES.index(n)
            for c in range(18):
                mix_out[ph, k, c] = jnp.where(low, flip(mixed_z[k, c, 1]), mixed_z[k, c, 2])
            remote(ph, "mz" + str(n)).start()

        def seen_z(n, slot):
            k = LANES.index(n)
            remote(ph, "mz" + str(n)).wait_recv()
            for c in range(18):
                edge = mix_in[ph, k, c]
                mixed_z[k, c, 0] = jnp.where(low, edge, flip(mixed_z[k, c, 1]))
                mixed_z[k, c, 1] = jnp.where(low, flip(edge), flip(mixed_z[k, c, 2]))

            def seen(x):
                m, c = load_matrix(mixed_z, (k,), x), load_matrix(field, (n,), x)
                if ph == 1 and slot is not None:
                    traces[slot + x] = real_trace(m, c)
                for p, value in enumerate(twice_traceless(m, c) if n == 3 else twice_traceless(c, m)):
                    lower_z[k, p, x] = value
            loop(2, seen)

        def ahead_z(m):
            for c in range(18):
                edge = lane_in[ph, LANES.index(m), c]
                lane_ahead[m, c, 0] = jnp.where(low, lane_ahead[m, c, 0], edge)
                lane_ahead[m, c, 1] = jnp.where(low, lane_ahead[m, c, 1], flip(edge))

        loop(2, lambda x: shift_time(2, x))
        loop(2, lambda x: mix_z(3, x, load_matrix(time_ahead, (2,), x)))
        send_mixed(3)
        pack_lanes(ph, 3)
        remote(ph, "z3").start()
        if ph == 1:
            pl.semaphore_wait(known_sem.at[0], 2)
            known(1, -4, 4)

        loop(4, lambda i: shift_time(i // 2, lax.rem(i, 2)))

        def mix_x(x):
            store_matrix(mixed_x, (ph,), (x + 1,), mix(0, 3, x, load_matrix(time_ahead, (0,), x)))
        loop(2, mix_x)
        remote(ph, "mx").start()

        remote(ph, "y").wait_recv()

        def shift_rows(i):
            k, x = i // 2, lax.rem(i, 2)
            n = k + (k + 1) // 2
            for c in range(18):
                v = field[n, c, x]
                edge = jnp.broadcast_to(row_in[ph, k, c, x], (8, 128))
                row_ahead[n, c, x] = jnp.where(last_row, edge, pltpu.roll(v, 7, 0))
        loop(6, shift_rows)
        loop(2, lambda x: mix_z(1, x, load_matrix(row_ahead, (2,), x)))
        send_mixed(1)
        remote(ph, "x2").wait_recv()
        for x in range(2):
            mix_z(0, x, ahead_x(ph, 2, x))
        send_mixed(0)

        plane(ph, 1, 0, 0, load_matrix(row_ahead, (0,), 0), ahead_x(ph, 1, 0), 0)
        loop(2, lambda x: plane(
            ph, 1, 3, x, load_matrix(row_ahead, (3,), x), load_matrix(time_ahead, (1,), x), 2 + x))
        remote(ph, "x1").wait_recv()
        plane(ph, 1, 0, 1, load_matrix(row_ahead, (0,), 1), ahead_x(ph, 1, 1), 1)
        remote(ph, "lx1").start()

        remote(ph, "mx").wait_recv()

        def seen_x(x):
            m, c = load_matrix(mixed_x, (ph,), x), load_matrix(field, (3,), x)
            if ph == 1:
                traces[6 + x] = real_trace(m, c)
            for p, value in enumerate(twice_traceless(m, c)):
                lower[ph, 0, 3, p, x] = value
        loop(2, seen_x)
        remote(ph, "tx").start()

        seen_z(3, 8)
        remote(ph, "z0").wait_recv()
        if ph == 0:
            known(0, -2, 2)
        ahead_z(0)
        for x in (1, 0):
            plane(ph, 2, 0, x, load_matrix(lane_ahead, (0,), x), ahead_x(ph, 2, x), 10 + x)
            if x == 1:
                remote(ph, "lx2").start()
        remote(ph, "z1").wait_recv()
        ahead_z(1)
        loop(2, lambda x: plane(
            ph, 2, 1, x, load_matrix(lane_ahead, (1,), x), load_matrix(row_ahead, (2,), x), 4 + x, split=ph == 1))
        if ph == 1:
            total = traces[0]
            for slot in range(1, 12):
                total = total + traces[slot]
            gather_z[my_z] = jnp.sum(total, axis=0, keepdims=True)
            pl.semaphore_wait(known_sem.at[1], 2)
            for offset in range(1, half):
                z_sum(offset).start()
            known(2, half)
            loop(2, lambda x: below(ph, 2, 1, x, [loops[2, 1, p, x] for p in range(8)]))
        for k, m in enumerate(ROWS):
            for p in range(8):
                for x in range(2):
                    low_row_out[ph, k, p, x] = lower[ph, 1, m, p, x + 1, 7:8, :]
        remote(ph, "ly").start()

        def own_x(x):
            t = conjugated(dagger(load_matrix(field, (0,), x)), [lower[ph, 0, 3, p, x + 1] for p in range(8)])
            for p in range(8):
                loops[3, 0, p, x] = t[p]
            for p, value in enumerate(conjugated(load_matrix(field, (3,), x), t)):
                lower[ph, 3, 0, p, x + 1] = value
        remote(ph, "tx").wait_recv()
        loop(2, own_x)
        if ph == 1:
            for offset in range(1, half):
                z_sum(offset).wait_recv()
            total = gather_z[0]
            for source in range(1, half):
                total = total + gather_z[source]
            gather_rest[my_rest] = total
            pl.semaphore_wait(known_sem.at[2], 1)
            for offset in rest:
                rest_sum(offset).start()
        seen_z(1, None)
        seen_z(0, None)
        remote(ph, "z3").wait_recv()
        ahead_z(3)
        loop(2, lambda x: plane(
            ph, 3, 2, x, load_matrix(time_ahead, (2,), x), load_matrix(lane_ahead, (3,), x), None))

        for name in ("lx1", "lx2", "ly"):
            remote(ph, name).wait_recv()
    def half_step(ph, m, x):
        total = [None] * 8
        for n in range(4):
            if n == m:
                continue
            lead = LEAD[min(m, n), max(m, n)]
            first, second = (m, n) if lead == m else (n, m)
            for p in range(8):
                here = loops[first, second, p, x]
                if n == 0:
                    below_value = lower[ph, 0, m, p, x]
                elif n == 1:
                    edge = jnp.broadcast_to(low_row_in[ph, ROWS.index(m), p, x], (8, 128))
                    below_value = jnp.where(first_row, edge, pltpu.roll(lower[ph, 1, m, p, x + 1], 1, 0))
                elif n == 2:
                    below_value = lower_z[LANES.index(m), p, x]
                else:
                    value = lower[ph, 3, m, p, x + 1]
                    below_value = jnp.where(first_time, pltpu.roll(value, 65, 1), pltpu.roll(value, 1, 1))
                total[p] = add(total[p], here - below_value if lead == m else below_value - here)
        return [moment[m, PARTS[p], x] - (0.5 * KICK) * total[p] for p in range(8)]

    for m in range(4):
        loads[m].wait()
    send_rows(0)
    pack_lanes(0, 0)
    pl.semaphore_wait(barrier, len(neighbours))
    for name in ("y", "x2", "z0"):
        remote(0, name).start()
    pack_lanes(0, 1)
    for name in ("z1", "x1"):
        remote(0, name).start()
    loads[4].start()
    first_half(0)
    loads[4].wait()
    for m in (2, 0, 3, 1):
        def update(x):
            h = half_step(0, m, x)
            for p in range(8):
                moment[m, PARTS[p], x] = h[p]
            u = cayley(h, 0.5 * STEP)
            store_matrix(new_links, (m,), (x,), product(u, load_matrix(old_links, (m,), x)))
        loop(2, update)
        if m == 2:
            remote(1, "x2").start()
        elif m == 3:
            send_rows(1)
            pack_lanes(1, 0)
            remote(1, "y").start()
            remote(1, "z0").start()
        elif m == 1:
            pack_lanes(1, 1)
            remote(1, "z1").start()
            remote(1, "x1").start()
    first_half(1)

    def finish(x):
        for m in range(4):
            h = half_step(1, m, x)
            for p in range(8):
                final[m, PARTS[p], x] = h[p]
            final[m, 17, x] = -(h[0] + h[1])
            for c, p in ((3, 2), (6, 4), (7, 6)):
                final[m, c, x] = -h[p]
                final[m, 9 + c, x] = h[p + 1]
            for c in (0, 4, 8):
                final[m, c, x] = jnp.zeros((8, 128), F32)
    loop(2, finish)

    for ph in range(2):
        for name in names:
            remote(ph, name).wait_send()
    for offset in range(1, half):
        z_sum(offset).wait_send()
    for offset in rest:
        rest_sum(offset).wait_send()
    for offset in rest:
        rest_sum(offset).wait_recv()
    total = gather_rest[0]
    for source in range(1, len(rest) + 1):
        total = total + gather_rest[source]
    volume = 72.0 * (2 * 8 * 128) * (sizes[0] * sizes[1] * sizes[2])
    plaquette[...] = jnp.broadcast_to(jnp.sum(total) * (4.0 / volume), (8, 128))


def solution(mesh):
    sizes = tuple(mesh.shape[name] for name in NAMES)
    spec = P(None, None, None, None, "gx", "gy", "zt")

    def step(gauge, momenta):
        shape = gauge.shape
        flat = (4, 18) + shape[4:]
        dma = pltpu.SemaphoreType.DMA
        vmem = pl.BlockSpec(memory_space=pltpu.VMEM)
        half = sizes[2] // 2
        others = sizes[0] * sizes[1] * 2
        tile = (8, 128)

        def scratch(*lead):
            return pltpu.VMEM(lead + tile, F32)

        def rows(*lead):
            return pltpu.VMEM(lead + (1, 128), F32)

        fields, plaquette = pl.pallas_call(
            lambda *refs: kernel(sizes, *refs),
            name="md_step",
            out_shape=(jax.ShapeDtypeStruct((2,) + flat, F32), jax.ShapeDtypeStruct((8, 128), F32)),
            in_specs=[pl.BlockSpec(memory_space=pltpu.HBM)] * 2,
            out_specs=(vmem, vmem),
            scratch_shapes=[
                scratch(4, 18, 2), scratch(4, 18, 2), scratch(3, 18, 2), scratch(4, 18, 2), scratch(4, 18, 2),
                scratch(2, 18, 3), scratch(3, 18, 3),
                scratch(4, 4, 8, 2), scratch(2, 4, 4, 8, 3), scratch(3, 8, 2),
                rows(2, 3, 18, 2), rows(2, 3, 18, 2), scratch(2, 2, 18), scratch(2, 3, 18), scratch(2, 3, 18),
                scratch(2, 3, 18), scratch(2, 3, 18),
                rows(2, 3, 8, 2), rows(2, 3, 8, 2),
                scratch(12), rows(half), rows(others),
                dma((5,)), dma((2, 14)), dma((2, 14)), dma((half,)), dma((half,)), dma((others,)), dma((others,)),
                pltpu.SemaphoreType.REGULAR((3,)),
            ],
            compiler_params=pltpu.CompilerParams(collective_id=0, has_side_effects=True, vmem_limit_bytes=48 * 1024 * 1024),
        )(*(pltpu.with_memory_space_constraint(a.reshape(flat), pltpu.HBM) for a in (gauge, momenta)))
        return fields[0].reshape(shape), fields[1].reshape(shape), plaquette[0, 0]

    return jax.shard_map(step, mesh=mesh, in_specs=(spec, spec), out_specs=(spec, spec, P()), check_vma=False)
```
